32 devices in a mesh: freq: 4 (over y, x), space: 8 (over z, core).
Axes of the slice: x: 2, y: 2, z: 4, core: 2. Of those that a mesh axis runs over, the one named last changes fastest.
Arguments:
- spectra: bfloat16 [64, 24576, 256], P('freq', 'space'), may hold values from -48 to 48, as said below
- weight: float32 [24576], P('space'), may hold values from 0.25 to 4
- partner: int32 [64], P('freq'), may hold values from 0 to 15
- counts: int32 [64], P('freq'), may hold values from 1 to 8
Outputs:
- modes: bfloat16 [64, 16, 24576], P('freq', None, 'space')
- energy: float32 [64, 8], P('freq')
- coherence: float32 [64, 2, 8, 8], P('freq')
The draws below stay inside these ranges and needn't reach their ends.
Inputs may be any that keep to these rules, and one draw needn't show every extreme that they name: spectra are finite Fourier coefficients.
All inputs are finite; a program needn't handle non-finite values.
Results may differ from the reference program's by a relative error of at most 0.0045.
Values may be sent and summed in bfloat16 or wider, within the bound.
A program may use at most 128 MiB of HBM per device.

```python
import math
import jax
import jax.numpy as jnp
from jax import lax

NB = 128
FG = 16
KMAX = 8
ITERS = 4
NF = 64
NP = 24576
N_FREQ = 4


shared_terms = 256


def draw_spectra(key, part):
    keys = jax.random.split(key, 4)
    scales = jnp.exp(jax.random.uniform(keys[0], (NF, 1, NB), jnp.float32, 0.0, math.log(4.0)))
    noise = jax.random.normal(keys[1], (NF, NP, 2 * NB), jnp.float32)
    amplitude = 0.6
    shared = jax.random.normal(keys[2], (NP, shared_terms), jnp.float32)
    mixing = jax.random.normal(keys[3], (NF, shared_terms, 2 * NB), jnp.float32) * (amplitude * math.sqrt(8.0 / shared_terms))
    common = jnp.einsum('pr,frc->fpc', shared, mixing)
    doubled = jnp.concatenate([scales, scales], axis=2)
    return jnp.clip(doubled * (noise + common), -48.0, 48.0).astype(jnp.bfloat16)


def touch_ends(result, rng, low, high):
    place = [jax.random.randint(jax.random.fold_in(rng, axis), (), 0, length) for axis, length in enumerate(result.shape)]
    longest = result.shape.index(max(result.shape))
    beside = place[:longest] + [(place[longest] + 1) % result.shape[longest]] + place[longest + 1:]
    return result.at[tuple(place)].set(low).at[tuple(beside)].set(high)


def block_scale(rng, shape, cuts, smallest, high):
    loudness = 1.0
    for position, shards_of in cuts:
        heights = jax.random.uniform(jax.random.fold_in(jax.random.fold_in(rng, 6), position), (shards_of,), jnp.float32, smallest / len(cuts), high / len(cuts))
        loudness = loudness * jnp.repeat(jnp.exp(heights), shape[position] // shards_of).reshape((-1,) + (1,) * (len(shape) - 1 - position))
    return loudness


def setup_inputs(seed: int = 0) -> dict:
    arg_keys = jax.random.split(jax.random.key(seed), 5)
    return {
        "spectra": draw_spectra(jax.random.fold_in(arg_keys[4], 71), 0),
        "weight": jnp.clip(jnp.exp(math.log(4.0) - 2.7725887 * jax.random.uniform(arg_keys[1], (NP,), jnp.float32) ** block_scale(arg_keys[1], (NP,), ((0, 8),), -0.2, 0.2)), 0.25, 4.0),
        "partner": touch_ends(jax.random.randint(arg_keys[2], (NF,), 0, FG), jax.random.fold_in(arg_keys[2], 1), 0, FG - 1).astype(jnp.int32),
        "counts": touch_ends(jax.random.randint(arg_keys[3], (NF,), 1, KMAX + 1), jax.random.fold_in(arg_keys[3], 1), 1, KMAX).astype(jnp.int32),
    }


def embed(gram_re, gram_im):
    top = jnp.concatenate([gram_re, -gram_im], axis=2)
    bottom = jnp.concatenate([gram_im, gram_re], axis=2)
    return jnp.concatenate([top, bottom], axis=1)

def apply_operator(operator, basis):
    return jnp.einsum('fkc,fdc->fkd', basis, operator, precision=lax.Precision.HIGHEST)

def orthonormal(vectors, half):
    done = []
    for index in range(vectors.shape[1]):
        vector = vectors[:, index, :]
        for earlier in done:
            early_re, early_im = (earlier[:, :half], earlier[:, half:])
            vec_re, vec_im = (vector[:, :half], vector[:, half:])
            proj_re = lax.optimization_barrier(jnp.sum(early_re * vec_re + early_im * vec_im, axis=1, keepdims=True))
            proj_im = lax.optimization_barrier(jnp.sum(early_re * vec_im - early_im * vec_re, axis=1, keepdims=True))
            new_re = vec_re - proj_re * early_re + proj_im * early_im
            new_im = vec_im - proj_re * early_im - proj_im * early_re
            vector = jnp.concatenate([new_re, new_im], axis=1)
        length = jnp.sqrt(lax.optimization_barrier(jnp.sum(vector * vector, axis=1, keepdims=True)) + 1e-06)
        done.append(vector / length)
    return jnp.stack(done, axis=1)

def solve(gram_re, gram_im):
    half = gram_re.shape[1]
    operator = embed(gram_re, gram_im)
    basis = jnp.broadcast_to(jnp.eye(KMAX, 2 * half, dtype=jnp.float32), (gram_re.shape[0], KMAX, 2 * half))
    for sweep in range(ITERS):
        basis = orthonormal(apply_operator(operator, basis), half)
    image = apply_operator(operator, basis)
    energy = lax.optimization_barrier(jnp.sum(basis * image, axis=2))
    return (basis, energy)

def coefficients(basis, energy, counts):
    half = basis.shape[2] // 2
    ranks = jnp.arange(KMAX, dtype=jnp.int32)[None, :]
    scale = jnp.where(ranks < counts[:, None], 1.0 / jnp.sqrt(energy + 1e-06), 0.0)[:, :, None]
    part_re, part_im = (basis[:, :, :half], basis[:, :, half:])
    upper = jnp.concatenate([part_re, -part_im], axis=2) * scale
    lower = jnp.concatenate([part_im, part_re], axis=2) * scale
    return jnp.concatenate([upper, lower], axis=1).astype(jnp.bfloat16)

def reference(spectra, weight, partner, counts):
    half = NB

    def moment(block):
        weighted = (weight[:, None] * block).astype(jnp.bfloat16)
        return jnp.dot(block.T, weighted, preferred_element_type=jnp.float32)
    moments = lax.map(moment, spectra)
    gram_re = (moments[:, :half, :half] + moments[:, half:, half:]) / NP
    gram_im = (moments[:, :half, half:] - moments[:, half:, :half]) / NP
    basis, energy = solve(gram_re, gram_im)
    coefficient = coefficients(basis, energy, counts)

    def project(pair):
        return jnp.dot(pair[0], pair[1].T, preferred_element_type=jnp.float32).astype(jnp.bfloat16)
    modes = lax.map(project, (coefficient, spectra))
    freqs = jnp.arange(NF, dtype=jnp.int32)
    source = (N_FREQ - 1 - freqs // FG) * FG + partner
    partner_modes = jnp.take(modes, source.astype(jnp.int32), axis=0)

    def cohere(pair):
        phi = pair[0].astype(jnp.float32)
        psi = pair[1].astype(jnp.float32)
        wphi = phi * weight[None, :]
        hi = lax.Precision.HIGHEST
        real_part = jnp.dot(wphi[:KMAX], psi[:KMAX].T, precision=hi) + jnp.dot(wphi[KMAX:], psi[KMAX:].T, precision=hi)
        imag_part = jnp.dot(wphi[:KMAX], psi[KMAX:].T, precision=hi) - jnp.dot(wphi[KMAX:], psi[:KMAX].T, precision=hi)
        return jnp.stack([real_part, imag_part], axis=0) / NP
    coherence = lax.map(cohere, (modes, partner_modes))
    return (modes, energy, coherence)
```

```python
import functools

import jax
import jax.numpy as jnp
from jax import lax
from jax.experimental import pallas as pl
from jax.experimental.pallas import tpu as pltpu
from jax.sharding import PartitionSpec as P

KMAX = 8
ROWS = 2 * KMAX
ITERS = 4
AHEAD = 4
EPS = 1e-06
LINK = jnp.bfloat16
MESH = pl.DeviceIdType.MESH
F32 = jnp.float32
BF16 = jnp.bfloat16


def dot(left, right, dims):
    return lax.dot_general(left, right, (dims, ((), ())), preferred_element_type=F32)


def split(value):
    high = value.astype(BF16)
    return high, (value - high.astype(F32)).astype(BF16)


def exclusive(left, right, size):
    result, bit = 0, 1
    while bit < size:
        result = result + bit * lax.rem(lax.div(left, bit) + lax.div(right, bit), 2)
        bit *= 2
    return result


def pack(moments, half):
    real = moments[:half, :half] + moments[half:, half:]
    imag = moments[:half, half:] - moments[half:, :half]
    row = lax.broadcasted_iota(jnp.int32, (half, half), 0)
    col = lax.broadcasted_iota(jnp.int32, (half, half), 1)
    return jnp.where(row <= col, real, imag)


def unpack(packed, half):
    row = lax.broadcasted_iota(jnp.int32, (half, half), 0)
    col = lax.broadcasted_iota(jnp.int32, (half, half), 1)
    other = packed.T
    real = jnp.where(row <= col, packed, other)
    imag = jnp.where(row > col, packed, jnp.where(row < col, -other, 0.0))
    return real, imag


def orthonormal(real, imag):
    shape = real.shape
    row = lax.broadcasted_iota(jnp.int32, shape, 0)

    def spread(value, k):
        return jnp.broadcast_to(value[k : k + 1, :], shape)

    table = []
    for k in range(KMAX):
        a_re, a_im = spread(real, k), spread(imag, k)
        s_re = jnp.sum(a_re * real + a_im * imag, axis=1, keepdims=True)
        s_im = jnp.sum(a_re * imag - a_im * real, axis=1, keepdims=True)
        table.append((jnp.broadcast_to(s_re, shape), jnp.broadcast_to(s_im, shape)))
    for k in range(KMAX):
        s_re, s_im = table[k]
        inverse = lax.rsqrt(jnp.maximum(spread(s_re, k), 0.0) + EPS)
        square = inverse * inverse
        a_re, a_im = spread(real, k), spread(imag, k)
        c_re, c_im = s_re * square, s_im * square
        later_re = real - c_re * a_re + c_im * a_im
        later_im = imag - c_re * a_im - c_im * a_re
        real = jnp.where(row > k, later_re, jnp.where(row == k, real * inverse, real))
        imag = jnp.where(row > k, later_im, jnp.where(row == k, imag * inverse, imag))
        factor = 1.0 + EPS * square
        d_re, d_im = c_re * factor, c_im * factor
        for m in range(k + 1, KMAX):
            m_re, m_im = spread(d_re, m), spread(d_im, m)
            t_re, t_im = table[m]
            table[m] = (
                t_re - (m_re * s_re + m_im * s_im),
                t_im - (m_re * s_im - m_im * s_re),
            )
    return real, imag


def apply_operator(operator, real, imag, half):
    high, low = split(jnp.concatenate([real, imag], axis=0))
    left = jnp.concatenate([high, high, low], axis=1)
    image = dot(left, operator, ((1,), (0,)))
    new_re = image[:KMAX, :half] + image[KMAX:, half:]
    new_im = image[KMAX:, :half] - image[:KMAX, half:]
    return new_re, new_im


def select(crosses, side, partner, groups):
    per = 128 // ROWS
    lane = lax.broadcasted_iota(jnp.int32, (ROWS, 128), 1)
    place = lax.rem(lax.broadcasted_iota(jnp.int32, (KMAX, 128), 1), ROWS)
    parts = []
    for first in range(0, groups, per):
        kept = jnp.zeros((ROWS, 128), F32)
        for f in range(first, first + per):
            block = crosses[side, partner[side, f]]
            kept = jnp.where(lax.div(lane, ROWS) == f - first, block[:, first * ROWS : first * ROWS + 128], kept)
        top, bottom = kept[:KMAX], kept[KMAX:]
        real = top + pltpu.roll(bottom, 128 - KMAX, 1)
        imag = pltpu.roll(bottom, KMAX, 1) - top
        parts.append(jnp.where(place < KMAX, real, imag))
    return jnp.concatenate(parts, axis=1)


def kernel(
    n_freq, n_space, spectra, weight_in, partner_in, counts_in,
    modes, energy_out, coherence_out,
    held, columns, weight, send, recv, coefs, energies, mirrored, scaled,
    crosses, partner_there, partials, arrived, partner, counts,
    load_sem, small_sem, gram_send, gram_recv, basis_send, basis_recv, energy_send, energy_recv,
    modes_send, modes_recv, partner_send, partner_recv, part_send, part_recv,
):
    groups, points, width = held.shape
    half = width // 2
    part = points // 2
    own = groups // n_space
    total = points * n_space
    band = lax.axis_index("freq")
    me = lax.axis_index("space")
    opposite = n_freq - 1 - band
    upper = jnp.where(band > opposite, 1, 0)
    mine = pl.multiple_of(upper * part, 128)
    theirs = pl.multiple_of((1 - upper) * part, 128)

    def owner_of(step):
        return exclusive(me, n_space - 1 - lax.rem(step, n_space), n_space)

    def order(step):
        return lax.div(step, n_space) * n_space + owner_of(step)

    def load(step):
        f = order(step)
        return pltpu.make_async_copy(spectra.at[f], held.at[f], load_sem.at[f])

    weight_copy = pltpu.make_async_copy(weight_in, weight, small_sem.at[0])
    weight_copy.start()
    for step in range(min(AHEAD, groups)):
        load(step).start()

    barrier = pltpu.get_barrier_semaphore()
    for apart in range(1, n_space):
        peer = lax.rem(me + apart, n_space)
        pl.semaphore_signal(barrier, inc=1, device_id=(band, peer), device_id_type=MESH)
    for apart in range(n_space):
        peer = lax.rem(me + apart, n_space)
        pl.semaphore_signal(barrier, inc=1, device_id=(opposite, peer), device_id_type=MESH)

    mine_copy = pltpu.make_async_copy(partner_in, partner.at[pl.ds(0, 1)], small_sem.at[1])
    counts_copy = pltpu.make_async_copy(counts_in, counts, small_sem.at[2])
    mine_copy.start()
    counts_copy.start()
    weight_copy.wait()
    for block in range(points // 128):
        span = pl.ds(block * 128, 128)
        columns[span, :] = jnp.broadcast_to(weight[:, span], (128, 128)).T

    def moments_of(step):
        f = order(step)

        @pl.when(step + AHEAD < groups)
        def _():
            load(step + AHEAD).start()

        load(step).wait()
        block = held[f]
        scale = columns[...]
        weighted = (jnp.concatenate([scale, scale], axis=1) * block.astype(F32)).astype(BF16)
        return pack(dot(block, weighted, ((0,), (0,))), half).astype(LINK)

    def gram_copy(f, source, peer):
        return pltpu.make_async_remote_copy(
            src_ref=send.at[f], dst_ref=recv.at[lax.div(f, n_space), source], send_sem=gram_send.at[f],
            recv_sem=gram_recv.at[lax.div(f, n_space), source], device_id=(band, peer), device_id_type=MESH,
        )

    def gram_step(step, carry):
        f, owner = order(step), owner_of(step)
        packed = moments_of(step)

        @pl.when(owner != me)
        def _():
            send[f] = packed
            gram_copy(f, me, owner).start()

        @pl.when(owner == me)
        def _():
            recv[lax.div(f, n_space), me] = packed

        return carry

    first = order(0)
    send[first] = moments_of(0)
    pl.semaphore_wait(barrier, 2 * n_space - 1)
    gram_copy(first, me, owner_of(0)).start()
    partner_copy = pltpu.make_async_remote_copy(
        src_ref=partner_in, dst_ref=partner_there, send_sem=partner_send,
        recv_sem=partner_recv, device_id=(opposite, me), device_id_type=MESH,
    )
    partner_copy.start()
    mine_copy.wait()
    counts_copy.wait()

    ahead = n_space + n_space // 2 if own > 1 else n_space
    lax.fori_loop(1, ahead, gram_step, 0)

    def basis_copy(f, peer):
        return pltpu.make_async_remote_copy(
            src_ref=coefs.at[f], dst_ref=coefs.at[f], send_sem=basis_send.at[lax.div(f, n_space), peer],
            recv_sem=basis_recv.at[f], device_id=(band, peer), device_id_type=MESH,
        )

    def energy_copy(f, peer):
        return pltpu.make_async_remote_copy(
            src_ref=energies.at[f], dst_ref=energies.at[f], send_sem=energy_send.at[lax.div(f, n_space), peer],
            recv_sem=energy_recv.at[f], device_id=(band, peer), device_id_type=MESH,
        )

    def solve(slot):
        f = slot * n_space + me
        for apart in range(1, n_space):
            source = lax.rem(me + apart, n_space)
            gram_copy(f, source, source).wait_recv()
        packed = recv[slot, 0].astype(F32)
        for source in range(1, n_space):
            packed = packed + recv[slot, source].astype(F32)
        real, imag = unpack(packed / total, half)
        high, low = split(jnp.concatenate([real, imag], axis=1))
        operator = jnp.concatenate([high, low, high], axis=0)
        real, imag = orthonormal(real[:KMAX], -imag[:KMAX])
        for _ in range(ITERS - 1):
            real, imag = orthonormal(*apply_operator(operator, real, imag, half))
        image_re, image_im = apply_operator(operator, real, imag, half)
        energy = jnp.sum(real * image_re + imag * image_im, axis=1, keepdims=True)
        energy = jnp.broadcast_to(energy, (KMAX, half))
        rank = lax.broadcasted_iota(jnp.int32, (KMAX, half), 0)
        scale = jnp.where(rank < counts[0, f], 1.0 / jnp.sqrt(energy + EPS), 0.0)
        coefs[f] = jnp.concatenate([real * scale, imag * scale], axis=0).astype(BF16)
        energies[f] = energy
        for apart in range(1, n_space):
            basis_copy(f, exclusive(me, n_space - apart, n_space)).start()
        for apart in range(1, n_space):
            energy_copy(f, exclusive(me, n_space - apart, n_space)).start()

    def modes_copy(f):
        return pltpu.make_async_remote_copy(
            src_ref=modes.at[f, :, pl.ds(theirs, part)], dst_ref=mirrored.at[f],
            send_sem=modes_send.at[f], recv_sem=modes_recv.at[f],
            device_id=(opposite, me), device_id_type=MESH,
        )

    def modes_step(slot, step):
        source = exclusive(me, step, n_space)
        f = slot * n_space + source

        @pl.when(step > 0)
        def _():
            basis_copy(f, source).wait_recv()

        basis = coefs[f].astype(F32)
        real, imag = basis[:KMAX], basis[KMAX:]
        coefficient = jnp.concatenate(
            [jnp.concatenate([real, -imag], axis=1), jnp.concatenate([imag, real], axis=1)], axis=0
        ).astype(BF16)
        modes[f] = dot(coefficient, held[f], ((1,), (1,))).astype(BF16)
        modes_copy(f).start()
        weighted = modes[f, :, pl.ds(mine, part)].astype(F32) * weight[:, pl.ds(mine, part)]
        high, low = split(weighted)
        scaled[0, f] = high
        scaled[1, f] = low

    for slot in range(own):
        solve(slot)
        rest = groups - ahead if slot == 0 else 0

        def both(step, carry, slot=slot):
            modes_step(slot, step)
            return gram_step(ahead + step, carry)

        def alone(step, carry, slot=slot):
            modes_step(slot, step)
            return carry

        mixed = min(rest, n_space)
        if mixed:
            lax.fori_loop(0, mixed, both, 0)
        if rest > mixed:
            lax.fori_loop(ahead + mixed, groups, gram_step, 0)
        if mixed < n_space:
            lax.fori_loop(mixed, n_space, alone, 0)

    partner_copy.wait()
    there_copy = pltpu.make_async_copy(partner_there, partner.at[pl.ds(1, 1)], small_sem.at[1])
    there_copy.start()

    lane = lax.broadcasted_iota(jnp.int32, (KMAX, half), 1)
    gathered = jnp.zeros((KMAX, half), F32)
    for f in range(groups):
        slot, source = f // n_space, f % n_space

        @pl.when(source != me)
        def _(f=f, source=source):
            energy_copy(f, source).wait_recv()

        gathered = jnp.where(lane == f, energies[f], gathered)
    energy_out[...] = gathered
    there_copy.wait()

    def modes_wait(f, carry):
        modes_copy(f).wait_recv()
        return carry

    lax.fori_loop(0, groups, modes_wait, 0)
    wide = groups * ROWS
    psi = mirrored[...].reshape(wide, part)
    cross = dot(scaled[0].reshape(wide, part), psi, ((1,), (1,)))
    cross = (cross + dot(scaled[1].reshape(wide, part), psi, ((1,), (1,)))) / total
    crosses[0] = cross.T.reshape(groups, ROWS, wide)
    crosses[1] = cross.reshape(groups, ROWS, wide)
    partials[1] = select(crosses, 1, partner, groups)
    partials[0] = select(crosses, 0, partner, groups)

    def part_copy(side, source, peer):
        across = opposite if side else band
        return pltpu.make_async_remote_copy(
            src_ref=partials.at[side], dst_ref=arrived.at[side, source],
            send_sem=part_send.at[side, peer], recv_sem=part_recv.at[side, source],
            device_id=(across, peer), device_id_type=MESH,
        )

    for apart in range(n_space - 1, -1, -1):
        peer = exclusive(me, apart, n_space)
        part_copy(1, me, peer).start()
        if apart:
            part_copy(0, me, peer).start()

    def drain(f, carry):
        modes_copy(f).wait_send()
        return carry

    lax.fori_loop(0, groups, drain, 0)
    for step in range(groups):
        f = order(step)
        if step % n_space != n_space - 1:
            gram_copy(f, me, me).wait_send()
    for slot in range(own):
        for apart in range(1, n_space):
            peer = exclusive(me, apart, n_space)
            basis_copy(slot * n_space + me, peer).wait_send()
            energy_copy(slot * n_space + me, peer).wait_send()

    result = partials[0]
    for apart in range(n_space):
        peer = exclusive(me, apart, n_space)
        part_copy(1, peer, peer).wait()
        result = result + arrived[1, peer]
        if apart:
            part_copy(0, peer, peer).wait()
            result = result + arrived[0, peer]
    coherence_out[...] = result


def finish(modes, energy, coherence, modes_out, energy_out, coherence_out, few, blocks, sems):
    groups = energy_out.shape[1]
    wide = groups * ROWS
    modes_copy = pltpu.make_async_copy(modes, modes_out, sems.at[2])
    modes_copy.start()
    few[...] = energy[:, :groups]
    energy_copy = pltpu.make_async_copy(few, energy_out, sems.at[0])
    energy_copy.start()
    value = coherence[...]
    high, low = split(value)
    lowest = (value - high.astype(F32) - low.astype(F32)).astype(BF16)
    row = lax.broadcasted_iota(jnp.int32, (wide, wide), 0)
    col = lax.broadcasted_iota(jnp.int32, (wide, wide), 1)
    source = lax.rem(col, groups) * ROWS + lax.div(col, groups)
    move = jnp.where(row == source, 1.0, 0.0).astype(BF16)
    moved = dot(high, move, ((1,), (0,))) + dot(low, move, ((1,), (0,))) + dot(lowest, move, ((1,), (0,)))
    for place in range(ROWS):
        blocks[place] = moved[:, place * groups : (place + 1) * groups]
    coherence_copy = pltpu.make_async_copy(blocks, coherence_out, sems.at[1])
    coherence_copy.start()
    energy_copy.wait()
    coherence_copy.wait()
    modes_copy.wait()


def on_device(n_freq, n_space, spectra, weight, partner, counts):
    groups, points, width = spectra.shape
    half = width // 2
    own = groups // n_space
    wide = groups * ROWS
    dma = pltpu.SemaphoreType.DMA
    vmem = pl.BlockSpec(memory_space=pltpu.VMEM)
    hbm = pl.BlockSpec(memory_space=pltpu.HBM)
    modes, energy, coherence = pl.pallas_call(
        functools.partial(kernel, n_freq, n_space),
        out_shape=(
            pltpu.VMEM((groups, ROWS, points), BF16),
            pltpu.VMEM((KMAX, half), F32),
            pltpu.VMEM((KMAX, wide), F32),
        ),
        in_specs=[hbm, hbm, hbm, hbm],
        out_specs=(vmem, vmem, vmem),
        scratch_shapes=[
            pltpu.VMEM((groups, points, width), BF16),
            pltpu.VMEM((points, 128), F32),
            pltpu.VMEM((1, points), F32),
            pltpu.VMEM((groups, half, half), LINK),
            pltpu.VMEM((own, n_space, half, half), LINK),
            pltpu.VMEM((groups, ROWS, half), BF16),
            pltpu.VMEM((groups, KMAX, half), F32),
            pltpu.VMEM((groups, ROWS, points // 2), BF16),
            pltpu.VMEM((2, groups, ROWS, points // 2), BF16),
            pltpu.VMEM((2, groups, ROWS, wide), F32),
            pltpu.VMEM((1, groups), jnp.int32),
            pltpu.VMEM((2, KMAX, wide), F32),
            pltpu.VMEM((2, n_space, KMAX, wide), F32),
            pltpu.SMEM((2, groups), jnp.int32),
            pltpu.SMEM((1, groups), jnp.int32),
            dma((groups,)),
            dma((3,)),
            dma((groups,)),
            dma((own, n_space)),
            dma((own, n_space)),
            dma((groups,)),
            dma((own, n_space)),
            dma((groups,)),
            dma((groups,)),
            dma((groups,)),
            dma(()),
            dma(()),
            dma((2, n_space)),
            dma((2, n_space)),
        ],
        compiler_params=pltpu.CompilerParams(
            collective_id=0, has_side_effects=True, vmem_limit_bytes=60 * 1024 * 1024
        ),
    )(spectra, weight.reshape(1, points), partner.reshape(1, groups), counts.reshape(1, groups))
    modes = pltpu.with_memory_space_constraint(modes, pltpu.VMEM)
    energy = pltpu.with_memory_space_constraint(energy, pltpu.VMEM)
    coherence = pltpu.with_memory_space_constraint(coherence, pltpu.VMEM)
    modes, energy, coherence = pl.pallas_call(
        finish,
        out_shape=(
            jax.ShapeDtypeStruct((groups, ROWS, points), BF16),
            jax.ShapeDtypeStruct((KMAX, groups), F32),
            jax.ShapeDtypeStruct((ROWS, KMAX, groups), F32),
        ),
        in_specs=[vmem, vmem, vmem],
        out_specs=(hbm, hbm, hbm),
        scratch_shapes=[
            pltpu.VMEM((KMAX, groups), F32),
            pltpu.VMEM((ROWS, KMAX, groups), F32),
            dma((3,)),
        ],
    )(modes, energy, coherence)
    coherence = coherence.reshape(2, KMAX, KMAX, groups).transpose(3, 0, 1, 2)
    return modes, energy.T, coherence


def solution(mesh):
    in_specs = (P("freq", "space", None), P("space"), P("freq"), P("freq"))
    out_specs = (P("freq", None, "space"), P("freq", None), P("freq", None, None, None))
    return jax.shard_map(
        functools.partial(on_device, mesh.shape["freq"], mesh.shape["space"]),
        mesh=mesh,
        in_specs=in_specs,
        out_specs=out_specs,
        check_vma=False,
    )
```

```python
import functools

import jax
import jax.numpy as jnp
from jax import lax
from jax.experimental import pallas as pl
from jax.experimental.pallas import tpu as pltpu
from jax.sharding import PartitionSpec as P

KMAX = 8
ROWS = 2 * KMAX
ITERS = 4
AHEAD = 4
EPS = 1e-06
LINK = jnp.bfloat16
MESH = pl.DeviceIdType.MESH
F32 = jnp.float32
BF16 = jnp.bfloat16


def dot(left, right, dims):
    return lax.dot_general(left, right, (dims, ((), ())), preferred_element_type=F32)


def split(value):
    high = value.astype(BF16)
    return high, (value - high.astype(F32)).astype(BF16)


def exclusive(left, right, size):
    result, bit = 0, 1
    while bit < size:
        result = result + bit * lax.rem(lax.div(left, bit) + lax.div(right, bit), 2)
        bit *= 2
    return result


def pack(moments, half):
    real = moments[:half, :half] + moments[half:, half:]
    imag = moments[:half, half:] - moments[half:, :half]
    row = lax.broadcasted_iota(jnp.int32, (half, half), 0)
    col = lax.broadcasted_iota(jnp.int32, (half, half), 1)
    return jnp.where(row <= col, real, imag)


def unpack(packed, half):
    row = lax.broadcasted_iota(jnp.int32, (half, half), 0)
    col = lax.broadcasted_iota(jnp.int32, (half, half), 1)
    other = packed.T
    real = jnp.where(row <= col, packed, other)
    imag = jnp.where(row > col, packed, jnp.where(row < col, -other, 0.0))
    return real, imag


def orthonormal(real, imag):
    shape = real.shape
    row = lax.broadcasted_iota(jnp.int32, shape, 0)

    def spread(value, k):
        return jnp.broadcast_to(value[k : k + 1, :], shape)

    table = []
    for k in range(KMAX):
        a_re, a_im = spread(real, k), spread(imag, k)
        s_re = jnp.sum(a_re * real + a_im * imag, axis=1, keepdims=True)
        s_im = jnp.sum(a_re * imag - a_im * real, axis=1, keepdims=True)
        table.append((jnp.broadcast_to(s_re, shape), jnp.broadcast_to(s_im, shape)))
    for k in range(KMAX):
        s_re, s_im = table[k]
        inverse = lax.rsqrt(jnp.maximum(spread(s_re, k), 0.0) + EPS)
        square = inverse * inverse
        a_re, a_im = spread(real, k), spread(imag, k)
        c_re, c_im = s_re * square, s_im * square
        later_re = real - c_re * a_re + c_im * a_im
        later_im = imag - c_re * a_im - c_im * a_re
        real = jnp.where(row > k, later_re, jnp.where(row == k, real * inverse, real))
        imag = jnp.where(row > k, later_im, jnp.where(row == k, imag * inverse, imag))
        factor = 1.0 + EPS * square
        d_re, d_im = c_re * factor, c_im * factor
        for m in range(k + 1, KMAX):
            m_re, m_im = spread(d_re, m), spread(d_im, m)
            t_re, t_im = table[m]
            table[m] = (
                t_re - (m_re * s_re + m_im * s_im),
                t_im - (m_re * s_im - m_im * s_re),
            )
    return real, imag


def apply_operator(operator, real, imag, half):
    high, low = split(jnp.concatenate([real, imag], axis=0))
    left = jnp.concatenate([high, high, low], axis=1)
    image = dot(left, operator, ((1,), (0,)))
    new_re = image[:KMAX, :half] + image[KMAX:, half:]
    new_im = image[KMAX:, :half] - image[:KMAX, half:]
    return new_re, new_im


def select(crosses, side, partner, groups):
    per = 128 // ROWS
    lane = lax.broadcasted_iota(jnp.int32, (ROWS, 128), 1)
    place = lax.rem(lax.broadcasted_iota(jnp.int32, (KMAX, 128), 1), ROWS)
    parts = []
    for first in range(0, groups, per):
        kept = jnp.zeros((ROWS, 128), F32)
        for f in range(first, first + per):
            block = crosses[side, partner[side, f]]
            kept = jnp.where(lax.div(lane, ROWS) == f - first, block[:, first * ROWS : first * ROWS + 128], kept)
        top, bottom = kept[:KMAX], kept[KMAX:]
        real = top + pltpu.roll(bottom, 128 - KMAX, 1)
        imag = pltpu.roll(bottom, KMAX, 1) - top
        parts.append(jnp.where(place < KMAX, real, imag))
    return jnp.concatenate(parts, axis=1)


def kernel(
    n_freq, n_space, spectra, weight_in, partner_in, counts_in,
    modes, energy_out, coherence_out,
    ring, held, weight, relay, relayed, kept, send, recv, mine_sum, coefs, energies, mirrored, scaled,
    crosses, partner_there, partials, arrived, partner, counts,
    load_sem, small_sem, relay_send, relay_recv, gram_send, gram_recv, basis_send, basis_recv,
    energy_send, energy_recv, modes_send, modes_recv, partner_send, partner_recv, part_send, part_recv,
):
    groups, width, points = held.shape
    half = width // 2
    part = points // 2
    own = groups // n_space
    chips = n_space // 2
    wide = groups * ROWS
    total = points * n_space
    band = lax.axis_index("freq")
    me = lax.axis_index("space")
    opposite = n_freq - 1 - band
    beside = exclusive(me, 1, n_space)
    upper = jnp.where(band > opposite, 1, 0)
    mine = pl.multiple_of(upper * part, 128)
    theirs = pl.multiple_of((1 - upper) * part, 128)

    def order(step):
        owner = exclusive(me, n_space - 1 - lax.rem(step, n_space), n_space)
        return lax.div(step, n_space) * n_space + owner

    def load(step):
        place = lax.rem(step, AHEAD)
        return pltpu.make_async_copy(spectra.at[order(step)], ring.at[place], load_sem.at[place])

    weight_copy = pltpu.make_async_copy(weight_in, weight, small_sem.at[0])
    weight_copy.start()
    for step in range(AHEAD):
        load(step).start()

    barrier = pltpu.get_barrier_semaphore()
    for apart in range(1, n_space):
        peer = lax.rem(me + apart, n_space)
        pl.semaphore_signal(barrier, inc=1, device_id=(band, peer), device_id_type=MESH)
    for apart in range(n_space):
        peer = lax.rem(me + apart, n_space)
        pl.semaphore_signal(barrier, inc=1, device_id=(opposite, peer), device_id_type=MESH)

    mine_copy = pltpu.make_async_copy(partner_in, partner.at[pl.ds(0, 1)], small_sem.at[1])
    counts_copy = pltpu.make_async_copy(counts_in, counts, small_sem.at[2])
    mine_copy.start()
    counts_copy.start()
    weight_copy.wait()

    def gram_pair(pair):
        packed = []
        for step in (2 * pair, 2 * pair + 1):
            load(step).wait()
        for step in (2 * pair, 2 * pair + 1):
            block = ring[lax.rem(step, AHEAD)]
            flipped = block.T
            held[order(step)] = flipped
            weighted = (flipped.astype(F32) * weight[...]).astype(BF16)
            packed.append(pack(dot(weighted, block, ((1,), (0,))), half))
        relay[pair] = packed[0]
        kept[pair] = packed[1]

        @pl.when(2 * pair + AHEAD < groups)
        def _():
            load(2 * pair + AHEAD).start()
            load(2 * pair + 1 + AHEAD).start()

    def relay_copy(pair):
        return pltpu.make_async_remote_copy(
            src_ref=relay.at[pair], dst_ref=relayed.at[pair], send_sem=relay_send,
            recv_sem=relay_recv.at[pair], device_id=(band, beside), device_id_type=MESH,
        )

    def gram_copy(slot, place):
        peer = exclusive(me, n_space - 2 - 2 * place, n_space)
        return pltpu.make_async_remote_copy(
            src_ref=send.at[slot, place], dst_ref=recv.at[slot, place], send_sem=gram_send,
            recv_sem=gram_recv.at[slot], device_id=(band, peer), device_id_type=MESH,
        )

    def forward(pair):
        slot, place = lax.div(pair, chips), lax.rem(pair, chips)
        relay_copy(pair).wait_recv()
        chip = kept[pair] + relayed[pair]

        @pl.when(place < chips - 1)
        def _():
            send[slot, place] = chip.astype(LINK)
            gram_copy(slot, place).start()

        @pl.when(place == chips - 1)
        def _():
            mine_sum[slot] = chip

    def gram_step(pair, carry):
        gram_pair(pair)
        relay_copy(pair).start()
        forward(pair - 1)
        return carry

    gram_pair(0)
    pl.semaphore_wait(barrier, 2 * n_space - 1)
    relay_copy(0).start()
    partner_copy = pltpu.make_async_remote_copy(
        src_ref=partner_in, dst_ref=partner_there, send_sem=partner_send,
        recv_sem=partner_recv, device_id=(opposite, me), device_id_type=MESH,
    )
    partner_copy.start()
    mine_copy.wait()
    counts_copy.wait()

    pairs = own * chips
    rest = chips // 2 if own > 1 else 0
    lax.fori_loop(1, pairs - rest, gram_step, 0)
    if not rest:
        forward(pairs - 1)

    def basis_copy(f, peer):
        return pltpu.make_async_remote_copy(
            src_ref=coefs.at[f], dst_ref=coefs.at[f], send_sem=basis_send,
            recv_sem=basis_recv.at[f], device_id=(band, peer), device_id_type=MESH,
        )

    def energy_copy(span, peer):
        return pltpu.make_async_remote_copy(
            src_ref=energies.at[span], dst_ref=energies.at[span], send_sem=energy_send,
            recv_sem=energy_recv, device_id=(band, peer), device_id_type=MESH,
        )

    def solve(slot):
        f = slot * n_space + me
        pltpu.make_async_remote_copy(
            src_ref=send.at[slot], dst_ref=recv.at[slot], send_sem=gram_send,
            recv_sem=gram_recv.at[slot], device_id=(band, beside), device_id_type=MESH,
        ).wait_recv()
        packed = mine_sum[slot]
        for place in range(chips - 1):
            packed = packed + recv[slot, place].astype(F32)
        real, imag = unpack(packed / total, half)
        high, low = split(jnp.concatenate([real, imag], axis=1))
        operator = jnp.concatenate([high, low, high], axis=0)
        real, imag = orthonormal(real[:KMAX], -imag[:KMAX])
        for _ in range(ITERS - 1):
            real, imag = orthonormal(*apply_operator(operator, real, imag, half))
        image_re, image_im = apply_operator(operator, real, imag, half)
        energy = jnp.sum(real * image_re + imag * image_im, axis=1, keepdims=True)
        energy = jnp.broadcast_to(energy, (KMAX, half))
        rank = lax.broadcasted_iota(jnp.int32, (KMAX, half), 0)
        scale = jnp.where(rank < counts[0, f], 1.0 / jnp.sqrt(energy + EPS), 0.0)
        coefs[f] = jnp.concatenate([real * scale, imag * scale], axis=0).astype(BF16)
        energies[f] = energy
        for apart in range(1, n_space):
            basis_copy(f, exclusive(me, n_space - apart, n_space)).start()
        for apart in range(1, n_space):
            energy_copy(pl.ds(f, 1), exclusive(me, n_space - apart, n_space)).start()

    def modes_copy(f):
        return pltpu.make_async_remote_copy(
            src_ref=modes.at[f, :, pl.ds(theirs, part)], dst_ref=mirrored.at[f],
            send_sem=modes_send, recv_sem=modes_recv.at[lax.div(f, n_space)],
            device_id=(opposite, me), device_id_type=MESH,
        )

    def modes_step(slot, step):
        source = exclusive(me, step, n_space)
        f = slot * n_space + source

        @pl.when(step > 0)
        def _():
            basis_copy(f, source).wait_recv()

        basis = coefs[f].astype(F32)
        real, imag = basis[:KMAX], basis[KMAX:]
        coefficient = jnp.concatenate(
            [jnp.concatenate([real, -imag], axis=1), jnp.concatenate([imag, real], axis=1)], axis=0
        ).astype(BF16)
        modes[f] = dot(coefficient, held[f], ((1,), (0,))).astype(BF16)
        modes_copy(f).start()
        weighted = modes[f, :, pl.ds(mine, part)].astype(F32) * weight[:, pl.ds(mine, part)]
        high, low = split(weighted)
        scaled[0, f] = high
        scaled[1, f] = low

    for slot in range(own):
        solve(slot)

        def alone(step, carry, slot=slot):
            modes_step(slot, step)
            return carry

        if slot == 0 and rest:

            def both(turn, carry):
                lax.fori_loop(2 * turn, 2 * turn + 2, alone, 0)
                return gram_step(pairs - rest + turn, carry)

            lax.fori_loop(0, rest, both, 0)
            lax.fori_loop(2 * rest, 2 * rest + 2, alone, 0)
            forward(pairs - 1)
            lax.fori_loop(2 * rest + 2, n_space, alone, 0)
        else:
            lax.fori_loop(0, n_space, alone, 0)

    partner_copy.wait()
    there_copy = pltpu.make_async_copy(partner_there, partner.at[pl.ds(1, 1)], small_sem.at[1])
    there_copy.start()
    sent = pl.ds(0, own * (n_space - 1))
    energy_copy(sent, beside).wait()
    lane = lax.broadcasted_iota(jnp.int32, (KMAX, half), 1)
    gathered = jnp.zeros((KMAX, half), F32)
    for f in range(groups):
        gathered = jnp.where(lane == f, energies[f], gathered)
    energy_out[...] = gathered
    pltpu.make_async_remote_copy(
        src_ref=coefs.at[sent], dst_ref=coefs.at[sent], send_sem=basis_send,
        recv_sem=basis_recv.at[0], device_id=(band, beside), device_id_type=MESH,
    ).wait_send()
    pltpu.make_async_remote_copy(
        src_ref=relay, dst_ref=relayed, send_sem=relay_send,
        recv_sem=relay_recv.at[0], device_id=(band, beside), device_id_type=MESH,
    ).wait_send()
    pltpu.make_async_remote_copy(
        src_ref=send, dst_ref=recv, send_sem=gram_send,
        recv_sem=gram_recv.at[0], device_id=(band, beside), device_id_type=MESH,
    ).wait_send()
    there_copy.wait()

    for slot in range(own):
        span = pl.ds(slot * n_space, n_space)
        pltpu.make_async_remote_copy(
            src_ref=mirrored.at[span], dst_ref=mirrored.at[span], send_sem=modes_send,
            recv_sem=modes_recv.at[slot], device_id=(opposite, me), device_id_type=MESH,
        ).wait_recv()
        rows = n_space * ROWS
        psi = mirrored[span].reshape(rows, part)
        cross = dot(psi, scaled[0].reshape(wide, part), ((1,), (1,)))
        cross = (cross + dot(psi, scaled[1].reshape(wide, part), ((1,), (1,)))) / total
        crosses[0, span] = cross.reshape(n_space, ROWS, wide)
        crosses[1, :, :, slot * rows : (slot + 1) * rows] = cross.T.reshape(groups, ROWS, rows)
    partials[1] = select(crosses, 1, partner, groups)
    partials[0] = select(crosses, 0, partner, groups)

    def part_copy(side, peer):
        across = opposite if side else band
        return pltpu.make_async_remote_copy(
            src_ref=partials.at[side], dst_ref=arrived.at[side * n_space + me],
            send_sem=part_send, recv_sem=part_recv, device_id=(across, peer), device_id_type=MESH,
        )

    for apart in range(n_space - 1, -1, -1):
        peer = exclusive(me, apart, n_space)
        part_copy(1, peer).start()
        if apart:
            part_copy(0, peer).start()

    arrived[me] = partials[0]
    pltpu.make_async_remote_copy(
        src_ref=mirrored, dst_ref=mirrored, send_sem=modes_send,
        recv_sem=modes_recv.at[0], device_id=(opposite, me), device_id_type=MESH,
    ).wait_send()
    there = pl.ds(0, 2 * n_space - 1)
    pltpu.make_async_remote_copy(
        src_ref=arrived.at[there], dst_ref=arrived.at[there], send_sem=part_send,
        recv_sem=part_recv, device_id=(band, beside), device_id_type=MESH,
    ).wait()
    result = arrived[0]
    for place in range(1, 2 * n_space):
        result = result + arrived[place]
    coherence_out[...] = result


def finish(modes, energy, coherence, modes_out, energy_out, coherence_out, few, blocks, sems):
    groups = energy_out.shape[1]
    wide = groups * ROWS
    modes_copy = pltpu.make_async_copy(modes, modes_out, sems.at[2])
    modes_copy.start()
    few[...] = energy[:, :groups]
    energy_copy = pltpu.make_async_copy(few, energy_out, sems.at[0])
    energy_copy.start()
    value = coherence[...]
    high, low = split(value)
    lowest = (value - high.astype(F32) - low.astype(F32)).astype(BF16)
    row = lax.broadcasted_iota(jnp.int32, (wide, wide), 0)
    col = lax.broadcasted_iota(jnp.int32, (wide, wide), 1)
    source = lax.rem(col, groups) * ROWS + lax.div(col, groups)
    move = jnp.where(row == source, 1.0, 0.0).astype(BF16)
    moved = dot(high, move, ((1,), (0,))) + dot(low, move, ((1,), (0,))) + dot(lowest, move, ((1,), (0,)))
    for place in range(ROWS):
        blocks[place] = moved[:, place * groups : (place + 1) * groups]
    coherence_copy = pltpu.make_async_copy(blocks, coherence_out, sems.at[1])
    coherence_copy.start()
    energy_copy.wait()
    coherence_copy.wait()
    modes_copy.wait()


def on_device(n_freq, n_space, spectra, weight, partner, counts):
    groups, points, width = spectra.shape
    half = width // 2
    own = groups // n_space
    wide = groups * ROWS
    dma = pltpu.SemaphoreType.DMA
    vmem = pl.BlockSpec(memory_space=pltpu.VMEM)
    hbm = pl.BlockSpec(memory_space=pltpu.HBM)
    modes, energy, coherence = pl.pallas_call(
        functools.partial(kernel, n_freq, n_space),
        out_shape=(
            pltpu.VMEM((groups, ROWS, points), BF16),
            pltpu.VMEM((KMAX, half), F32),
            pltpu.VMEM((KMAX, wide), F32),
        ),
        in_specs=[hbm, hbm, hbm, hbm],
        out_specs=(vmem, vmem, vmem),
        scratch_shapes=[
            pltpu.VMEM((AHEAD, points, width), BF16),
            pltpu.VMEM((groups, width, points), BF16),
            pltpu.VMEM((1, points), F32),
            pltpu.VMEM((groups // 2, half, half), F32),
            pltpu.VMEM((groups // 2, half, half), F32),
            pltpu.VMEM((groups // 2, half, half), F32),
            pltpu.VMEM((own, n_space // 2 - 1, half, half), LINK),
            pltpu.VMEM((own, n_space // 2 - 1, half, half), LINK),
            pltpu.VMEM((own, half, half), F32),
            pltpu.VMEM((groups, ROWS, half), BF16),
            pltpu.VMEM((groups, KMAX, half), F32),
            pltpu.VMEM((groups, ROWS, points // 2), BF16),
            pltpu.VMEM((2, groups, ROWS, points // 2), BF16),
            pltpu.VMEM((2, groups, ROWS, wide), F32),
            pltpu.VMEM((1, groups), jnp.int32),
            pltpu.VMEM((2, KMAX, wide), F32),
            pltpu.VMEM((2 * n_space, KMAX, wide), F32),
            pltpu.SMEM((2, groups), jnp.int32),
            pltpu.SMEM((1, groups), jnp.int32),
            dma((AHEAD,)),
            dma((3,)),
            dma(()),
            dma((groups // 2,)),
            dma(()),
            dma((own,)),
            dma(()),
            dma((groups,)),
            dma(()),
            dma(()),
            dma(()),
            dma((own,)),
            dma(()),
            dma(()),
            dma(()),
            dma(()),
        ],
        compiler_params=pltpu.CompilerParams(
            collective_id=0, has_side_effects=True, vmem_limit_bytes=60 * 1024 * 1024
        ),
    )(spectra, weight.reshape(1, points), partner.reshape(1, groups), counts.reshape(1, groups))
    modes = pltpu.with_memory_space_constraint(modes, pltpu.VMEM)
    energy = pltpu.with_memory_space_constraint(energy, pltpu.VMEM)
    coherence = pltpu.with_memory_space_constraint(coherence, pltpu.VMEM)
    modes, energy, coherence = pl.pallas_call(
        finish,
        out_shape=(
            jax.ShapeDtypeStruct((groups, ROWS, points), BF16),
            jax.ShapeDtypeStruct((KMAX, groups), F32),
            jax.ShapeDtypeStruct((ROWS, KMAX, groups), F32),
        ),
        in_specs=[vmem, vmem, vmem],
        out_specs=(hbm, hbm, hbm),
        scratch_shapes=[
            pltpu.VMEM((KMAX, groups), F32),
            pltpu.VMEM((ROWS, KMAX, groups), F32),
            dma((3,)),
        ],
    )(modes, energy, coherence)
    coherence = coherence.reshape(2, KMAX, KMAX, groups).transpose(3, 0, 1, 2)
    return modes, energy.T, coherence


def solution(mesh):
    in_specs = (P("freq", "space", None), P("space"), P("freq"), P("freq"))
    out_specs = (P("freq", None, "space"), P("freq", None), P("freq", None, None, None))
    return jax.shard_map(
        functools.partial(on_device, mesh.shape["freq"], mesh.shape["space"]),
        mesh=mesh,
        in_specs=in_specs,
        out_specs=out_specs,
        check_vma=False,
    )
```

```python
import functools

import jax
import jax.numpy as jnp
from jax import lax
from jax.experimental import pallas as pl
from jax.experimental.pallas import tpu as pltpu
from jax.sharding import PartitionSpec as P

KMAX = 8
ROWS = 2 * KMAX
ITERS = 4
AHEAD = 6
EPS = 1e-06
LINK = jnp.bfloat16
MESH = pl.DeviceIdType.MESH
F32 = jnp.float32
BF16 = jnp.bfloat16


def dot(left, right, dims):
    return lax.dot_general(left, right, (dims, ((), ())), preferred_element_type=F32)


def split(value):
    high = value.astype(BF16)
    return high, (value - high.astype(F32)).astype(BF16)


def exclusive(left, right, size):
    result, bit = 0, 1
    while bit < size:
        result = result + bit * lax.rem(lax.div(left, bit) + lax.div(right, bit), 2)
        bit *= 2
    return result


def pack(moments, half):
    real = moments[:half, :half] + moments[half:, half:]
    imag = moments[:half, half:] - moments[half:, :half]
    row = lax.broadcasted_iota(jnp.int32, (half, half), 0)
    col = lax.broadcasted_iota(jnp.int32, (half, half), 1)
    return jnp.where(row <= col, real, imag)


def unpack(packed, half):
    row = lax.broadcasted_iota(jnp.int32, (half, half), 0)
    col = lax.broadcasted_iota(jnp.int32, (half, half), 1)
    other = packed.T
    real = jnp.where(row <= col, packed, other)
    imag = jnp.where(row > col, packed, jnp.where(row < col, -other, 0.0))
    return real, imag


def orthonormal(real, imag):
    shape = real.shape
    row = lax.broadcasted_iota(jnp.int32, shape, 0)

    def spread(value, k):
        return jnp.broadcast_to(value[k : k + 1, :], shape)

    table = []
    for k in range(KMAX):
        a_re, a_im = spread(real, k), spread(imag, k)
        s_re = jnp.sum(a_re * real + a_im * imag, axis=1, keepdims=True)
        s_im = jnp.sum(a_re * imag - a_im * real, axis=1, keepdims=True)
        table.append((jnp.broadcast_to(s_re, shape), jnp.broadcast_to(s_im, shape)))
    for k in range(KMAX):
        s_re, s_im = table[k]
        inverse = lax.rsqrt(jnp.maximum(spread(s_re, k), 0.0) + EPS)
        square = inverse * inverse
        a_re, a_im = spread(real, k), spread(imag, k)
        c_re, c_im = s_re * square, s_im * square
        later_re = real - c_re * a_re + c_im * a_im
        later_im = imag - c_re * a_im - c_im * a_re
        real = jnp.where(row > k, later_re, jnp.where(row == k, real * inverse, real))
        imag = jnp.where(row > k, later_im, jnp.where(row == k, imag * inverse, imag))
        factor = 1.0 + EPS * square
        d_re, d_im = c_re * factor, c_im * factor
        for m in range(k + 1, KMAX):
            m_re, m_im = spread(d_re, m), spread(d_im, m)
            t_re, t_im = table[m]
            table[m] = (
                t_re - (m_re * s_re + m_im * s_im),
                t_im - (m_re * s_im - m_im * s_re),
            )
    return real, imag


def apply_operator(operator, real, imag, half):
    high, low = split(jnp.concatenate([real, imag], axis=0))
    left = jnp.concatenate([high, high, low], axis=1)
    image = dot(left, operator, ((1,), (0,)))
    new_re = image[:KMAX, :half] + image[KMAX:, half:]
    new_im = image[KMAX:, :half] - image[:KMAX, half:]
    return new_re, new_im


def select(crosses, side, partner, groups):
    per = 128 // ROWS
    lane = lax.broadcasted_iota(jnp.int32, (ROWS, 128), 1)
    place = lax.rem(lax.broadcasted_iota(jnp.int32, (KMAX, 128), 1), ROWS)
    parts = []
    for first in range(0, groups, per):
        kept = jnp.zeros((ROWS, 128), F32)
        for f in range(first, first + per):
            block = crosses[side, partner[side, f]]
            kept = jnp.where(lax.div(lane, ROWS) == f - first, block[:, first * ROWS : first * ROWS + 128], kept)
        top, bottom = kept[:KMAX], kept[KMAX:]
        real = top + pltpu.roll(bottom, 128 - KMAX, 1)
        imag = pltpu.roll(bottom, KMAX, 1) - top
        parts.append(jnp.where(place < KMAX, real, imag))
    return jnp.concatenate(parts, axis=1)


def kernel(
    n_freq, n_space, spectra, weight_in, partner_in, counts_in,
    modes, energy_out, coherence_out,
    ring, held, weight, relay, relayed, kept, send, recv, mine_sum, coefs, energies, mirrored, scaled,
    crosses, partner_there, partials, arrived, partner, counts,
    load_sem, small_sem, relay_send, relay_recv, gram_send, gram_recv, basis_send, basis_recv,
    energy_send, energy_recv, modes_send, modes_recv, partner_send, partner_recv, part_send, part_recv,
):
    groups, width, points = held.shape
    half = width // 2
    part = points // 2
    own = groups // n_space
    chips = n_space // 2
    wide = groups * ROWS
    total = points * n_space
    band = lax.axis_index("freq")
    me = lax.axis_index("space")
    opposite = n_freq - 1 - band
    beside = exclusive(me, 1, n_space)
    upper = jnp.where(band > opposite, 1, 0)
    mine = pl.multiple_of(upper * part, 128)
    theirs = pl.multiple_of((1 - upper) * part, 128)

    def order(step):
        owner = exclusive(me, n_space - 1 - lax.rem(step, n_space), n_space)
        return lax.div(step, n_space) * n_space + owner

    def load(step):
        place = lax.rem(step, AHEAD)
        return pltpu.make_async_copy(spectra.at[order(step)], ring.at[place], load_sem.at[place])

    weight_copy = pltpu.make_async_copy(weight_in, weight, small_sem.at[0])
    weight_copy.start()
    for step in range(2):
        load(step).start()

    barrier = pltpu.get_barrier_semaphore()
    for apart in range(1, n_space):
        peer = lax.rem(me + apart, n_space)
        pl.semaphore_signal(barrier, inc=1, device_id=(band, peer), device_id_type=MESH)
    for apart in range(n_space):
        peer = lax.rem(me + apart, n_space)
        pl.semaphore_signal(barrier, inc=1, device_id=(opposite, peer), device_id_type=MESH)

    mine_copy = pltpu.make_async_copy(partner_in, partner.at[pl.ds(0, 1)], small_sem.at[1])
    counts_copy = pltpu.make_async_copy(counts_in, counts, small_sem.at[2])
    mine_copy.start()
    counts_copy.start()
    weight_copy.wait()
    for step in range(2, 4):
        load(step).start()

    def gram_pair(pair):
        packed = []
        for step in (2 * pair, 2 * pair + 1):
            load(step).wait()

        @pl.when(2 * pair + 4 < groups)
        def _():
            load(2 * pair + 4).start()
            load(2 * pair + 5).start()

        for step in (2 * pair, 2 * pair + 1):
            block = ring[lax.rem(step, AHEAD)]
            flipped = block.T
            held[order(step)] = flipped
            weighted = (flipped.astype(F32) * weight[...]).astype(BF16)
            packed.append(pack(dot(weighted, block, ((1,), (0,))), half))
        relay[pair] = packed[0]
        kept[pair] = packed[1]

    def relay_copy(pair):
        return pltpu.make_async_remote_copy(
            src_ref=relay.at[pair], dst_ref=relayed.at[pair], send_sem=relay_send,
            recv_sem=relay_recv.at[pair], device_id=(band, beside), device_id_type=MESH,
        )

    def gram_copy(slot, place):
        peer = exclusive(me, n_space - 2 - 2 * place, n_space)
        return pltpu.make_async_remote_copy(
            src_ref=send.at[slot, place], dst_ref=recv.at[slot, place], send_sem=gram_send,
            recv_sem=gram_recv.at[slot], device_id=(band, peer), device_id_type=MESH,
        )

    def forward(pair):
        slot, place = lax.div(pair, chips), lax.rem(pair, chips)
        relay_copy(pair).wait_recv()
        chip = kept[pair] + relayed[pair]

        @pl.when(place < chips - 1)
        def _():
            send[slot, place] = chip.astype(LINK)
            gram_copy(slot, place).start()

        @pl.when(place == chips - 1)
        def _():
            mine_sum[slot] = chip

    def gram_step(pair, carry):
        gram_pair(pair)
        relay_copy(pair).start()
        forward(pair - 1)
        return carry

    gram_pair(0)
    pl.semaphore_wait(barrier, 2 * n_space - 1)
    relay_copy(0).start()
    partner_copy = pltpu.make_async_remote_copy(
        src_ref=partner_in, dst_ref=partner_there, send_sem=partner_send,
        recv_sem=partner_recv, device_id=(opposite, me), device_id_type=MESH,
    )
    partner_copy.start()
    mine_copy.wait()
    counts_copy.wait()

    pairs = own * chips
    rest = chips // 2 if own > 1 else 0
    lax.fori_loop(1, pairs - rest, gram_step, 0)
    if not rest:
        forward(pairs - 1)

    def basis_copy(f, peer):
        return pltpu.make_async_remote_copy(
            src_ref=coefs.at[f], dst_ref=coefs.at[f], send_sem=basis_send,
            recv_sem=basis_recv.at[f], device_id=(band, peer), device_id_type=MESH,
        )

    def energy_copy(span, peer):
        return pltpu.make_async_remote_copy(
            src_ref=energies.at[span], dst_ref=energies.at[span], send_sem=energy_send,
            recv_sem=energy_recv, device_id=(band, peer), device_id_type=MESH,
        )

    def solve(slot):
        f = slot * n_space + me
        pltpu.make_async_remote_copy(
            src_ref=send.at[slot], dst_ref=recv.at[slot], send_sem=gram_send,
            recv_sem=gram_recv.at[slot], device_id=(band, beside), device_id_type=MESH,
        ).wait_recv()
        packed = mine_sum[slot]
        for place in range(chips - 1):
            packed = packed + recv[slot, place].astype(F32)
        real, imag = unpack(packed / total, half)
        high, low = split(jnp.concatenate([real, imag], axis=1))
        operator = jnp.concatenate([high, low, high], axis=0)
        real, imag = orthonormal(real[:KMAX], -imag[:KMAX])
        for _ in range(ITERS - 1):
            real, imag = orthonormal(*apply_operator(operator, real, imag, half))
        image_re, image_im = apply_operator(operator, real, imag, half)
        energy = jnp.sum(real * image_re + imag * image_im, axis=1, keepdims=True)
        energy = jnp.broadcast_to(energy, (KMAX, half))
        rank = lax.broadcasted_iota(jnp.int32, (KMAX, half), 0)
        scale = jnp.where(rank < counts[0, f], 1.0 / jnp.sqrt(energy + EPS), 0.0)
        coefs[f] = jnp.concatenate([real * scale, imag * scale], axis=0).astype(BF16)
        energies[f] = energy
        for apart in range(1, n_space):
            basis_copy(f, exclusive(me, n_space - apart, n_space)).start()
        for apart in range(1, n_space):
            energy_copy(pl.ds(f, 1), exclusive(me, n_space - apart, n_space)).start()

    def modes_copy(f):
        return pltpu.make_async_remote_copy(
            src_ref=modes.at[f, :, pl.ds(theirs, part)], dst_ref=mirrored.at[f],
            send_sem=modes_send, recv_sem=modes_recv.at[lax.div(f, n_space)],
            device_id=(opposite, me), device_id_type=MESH,
        )

    def modes_step(slot, step):
        source = exclusive(me, step, n_space)
        f = slot * n_space + source

        @pl.when(step > 0)
        def _():
            basis_copy(f, source).wait_recv()

        basis = coefs[f].astype(F32)
        real, imag = basis[:KMAX], basis[KMAX:]
        coefficient = jnp.concatenate(
            [jnp.concatenate([real, -imag], axis=1), jnp.concatenate([imag, real], axis=1)], axis=0
        ).astype(BF16)
        modes[f] = dot(coefficient, held[f], ((1,), (0,))).astype(BF16)
        modes_copy(f).start()
        weighted = modes[f, :, pl.ds(mine, part)].astype(F32) * weight[:, pl.ds(mine, part)]
        scaled[f] = weighted.astype(BF16)

    for slot in range(own):
        solve(slot)

        def alone(step, carry, slot=slot):
            modes_step(slot, step)
            return carry

        if slot == 0 and rest:

            def both(turn, carry):
                lax.fori_loop(2 * turn, 2 * turn + 2, alone, 0)
                return gram_step(pairs - rest + turn, carry)

            lax.fori_loop(0, rest, both, 0)
            lax.fori_loop(2 * rest, 2 * rest + 2, alone, 0)
            forward(pairs - 1)
            lax.fori_loop(2 * rest + 2, n_space, alone, 0)
        else:
            lax.fori_loop(0, n_space, alone, 0)

    partner_copy.wait()
    there_copy = pltpu.make_async_copy(partner_there, partner.at[pl.ds(1, 1)], small_sem.at[1])
    there_copy.start()
    sent = pl.ds(0, own * (n_space - 1))
    energy_copy(sent, beside).wait()
    lane = lax.broadcasted_iota(jnp.int32, (KMAX, half), 1)
    gathered = jnp.zeros((KMAX, half), F32)
    for f in range(groups):
        gathered = jnp.where(lane == f, energies[f], gathered)
    energy_out[...] = gathered
    pltpu.make_async_remote_copy(
        src_ref=coefs.at[sent], dst_ref=coefs.at[sent], send_sem=basis_send,
        recv_sem=basis_recv.at[0], device_id=(band, beside), device_id_type=MESH,
    ).wait_send()
    pltpu.make_async_remote_copy(
        src_ref=relay, dst_ref=relayed, send_sem=relay_send,
        recv_sem=relay_recv.at[0], device_id=(band, beside), device_id_type=MESH,
    ).wait_send()
    pltpu.make_async_remote_copy(
        src_ref=send, dst_ref=recv, send_sem=gram_send,
        recv_sem=gram_recv.at[0], device_id=(band, beside), device_id_type=MESH,
    ).wait_send()
    there_copy.wait()

    for slot in range(own):
        span = pl.ds(slot * n_space, n_space)
        pltpu.make_async_remote_copy(
            src_ref=mirrored.at[span], dst_ref=mirrored.at[span], send_sem=modes_send,
            recv_sem=modes_recv.at[slot], device_id=(opposite, me), device_id_type=MESH,
        ).wait_recv()
        rows = n_space * ROWS
        psi = mirrored[span].reshape(rows, part)
        cross = dot(scaled[...].reshape(wide, part), psi, ((1,), (1,))) / total
        crosses[0, span] = cross.T.reshape(n_space, ROWS, wide)
        crosses[1, :, :, slot * rows : (slot + 1) * rows] = cross.reshape(groups, ROWS, rows)
    partials[1] = select(crosses, 1, partner, groups).astype(LINK)
    partial = select(crosses, 0, partner, groups)
    partials[0] = partial.astype(LINK)

    def part_copy(side, peer):
        across = opposite if side else band
        return pltpu.make_async_remote_copy(
            src_ref=partials.at[side], dst_ref=arrived.at[side * n_space + me],
            send_sem=part_send, recv_sem=part_recv, device_id=(across, peer), device_id_type=MESH,
        )

    for apart in range(n_space - 1, -1, -1):
        peer = exclusive(me, apart, n_space)
        part_copy(1, peer).start()
        if apart:
            part_copy(0, peer).start()

    arrived[me] = jnp.zeros(arrived.shape[1:], LINK)
    pltpu.make_async_remote_copy(
        src_ref=mirrored, dst_ref=mirrored, send_sem=modes_send,
        recv_sem=modes_recv.at[0], device_id=(opposite, me), device_id_type=MESH,
    ).wait_send()
    there = pl.ds(0, 2 * n_space - 1)
    pltpu.make_async_remote_copy(
        src_ref=arrived.at[there], dst_ref=arrived.at[there], send_sem=part_send,
        recv_sem=part_recv, device_id=(band, beside), device_id_type=MESH,
    ).wait()
    result = partial
    for place in range(2 * n_space):
        result = result + arrived[place].astype(F32)
    coherence_out[...] = result


def finish(modes, energy, coherence, modes_out, energy_out, coherence_out, few, blocks, sems):
    groups = energy_out.shape[1]
    wide = groups * ROWS
    modes_copy = pltpu.make_async_copy(modes, modes_out, sems.at[2])
    modes_copy.start()
    few[...] = energy[:, :groups]
    energy_copy = pltpu.make_async_copy(few, energy_out, sems.at[0])
    energy_copy.start()
    value = coherence[...]
    high, low = split(value)
    lowest = (value - high.astype(F32) - low.astype(F32)).astype(BF16)
    row = lax.broadcasted_iota(jnp.int32, (wide, wide), 0)
    col = lax.broadcasted_iota(jnp.int32, (wide, wide), 1)
    source = lax.rem(col, groups) * ROWS + lax.div(col, groups)
    move = jnp.where(row == source, 1.0, 0.0).astype(BF16)
    moved = dot(high, move, ((1,), (0,))) + dot(low, move, ((1,), (0,))) + dot(lowest, move, ((1,), (0,)))
    for place in range(ROWS):
        blocks[place] = moved[:, place * groups : (place + 1) * groups]
    coherence_copy = pltpu.make_async_copy(blocks, coherence_out, sems.at[1])
    coherence_copy.start()
    energy_copy.wait()
    coherence_copy.wait()
    modes_copy.wait()


def on_device(n_freq, n_space, spectra, weight, partner, counts):
    groups, points, width = spectra.shape
    half = width // 2
    own = groups // n_space
    wide = groups * ROWS
    dma = pltpu.SemaphoreType.DMA
    vmem = pl.BlockSpec(memory_space=pltpu.VMEM)
    hbm = pl.BlockSpec(memory_space=pltpu.HBM)
    modes, energy, coherence = pl.pallas_call(
        functools.partial(kernel, n_freq, n_space),
        out_shape=(
            pltpu.VMEM((groups, ROWS, points), BF16),
            pltpu.VMEM((KMAX, half), F32),
            pltpu.VMEM((KMAX, wide), F32),
        ),
        in_specs=[hbm, hbm, hbm, hbm],
        out_specs=(vmem, vmem, vmem),
        scratch_shapes=[
            pltpu.VMEM((AHEAD, points, width), BF16),
            pltpu.VMEM((groups, width, points), BF16),
            pltpu.VMEM((1, points), F32),
            pltpu.VMEM((groups // 2, half, half), F32),
            pltpu.VMEM((groups // 2, half, half), F32),
            pltpu.VMEM((groups // 2, half, half), F32),
            pltpu.VMEM((own, n_space // 2 - 1, half, half), LINK),
            pltpu.VMEM((own, n_space // 2 - 1, half, half), LINK),
            pltpu.VMEM((own, half, half), F32),
            pltpu.VMEM((groups, ROWS, half), BF16),
            pltpu.VMEM((groups, KMAX, half), F32),
            pltpu.VMEM((groups, ROWS, points // 2), BF16),
            pltpu.VMEM((groups, ROWS, points // 2), BF16),
            pltpu.VMEM((2, groups, ROWS, wide), F32),
            pltpu.VMEM((1, groups), jnp.int32),
            pltpu.VMEM((2, KMAX, wide), LINK),
            pltpu.VMEM((2 * n_space, KMAX, wide), LINK),
            pltpu.SMEM((2, groups), jnp.int32),
            pltpu.SMEM((1, groups), jnp.int32),
            dma((AHEAD,)),
            dma((3,)),
            dma(()),
            dma((groups // 2,)),
            dma(()),
            dma((own,)),
            dma(()),
            dma((groups,)),
            dma(()),
            dma(()),
            dma(()),
            dma((own,)),
            dma(()),
            dma(()),
            dma(()),
            dma(()),
        ],
        compiler_params=pltpu.CompilerParams(
            collective_id=0, has_side_effects=True, vmem_limit_bytes=60 * 1024 * 1024
        ),
    )(spectra, weight.reshape(1, points), partner.reshape(1, groups), counts.reshape(1, groups))
    modes = pltpu.with_memory_space_constraint(modes, pltpu.VMEM)
    energy = pltpu.with_memory_space_constraint(energy, pltpu.VMEM)
    coherence = pltpu.with_memory_space_constraint(coherence, pltpu.VMEM)
    modes, energy, coherence = pl.pallas_call(
        finish,
        out_shape=(
            jax.ShapeDtypeStruct((groups, ROWS, points), BF16),
            jax.ShapeDtypeStruct((KMAX, groups), F32),
            jax.ShapeDtypeStruct((ROWS, KMAX, groups), F32),
        ),
        in_specs=[vmem, vmem, vmem],
        out_specs=(hbm, hbm, hbm),
        scratch_shapes=[
            pltpu.VMEM((KMAX, groups), F32),
            pltpu.VMEM((ROWS, KMAX, groups), F32),
            dma((3,)),
        ],
    )(modes, energy, coherence)
    coherence = coherence.reshape(2, KMAX, KMAX, groups).transpose(3, 0, 1, 2)
    return modes, energy.T, coherence


def solution(mesh):
    in_specs = (P("freq", "space", None), P("space"), P("freq"), P("freq"))
    out_specs = (P("freq", None, "space"), P("freq", None), P("freq", None, None, None))
    return jax.shard_map(
        functools.partial(on_device, mesh.shape["freq"], mesh.shape["space"]),
        mesh=mesh,
        in_specs=in_specs,
        out_specs=out_specs,
        check_vma=False,
    )
```

```python
import functools

import jax
import jax.numpy as jnp
from jax import lax
from jax.experimental import pallas as pl
from jax.experimental.pallas import tpu as pltpu
from jax.sharding import PartitionSpec as P

KMAX = 8
ROWS = 2 * KMAX
ITERS = 4
AHEAD = 6
EPS = 1e-06
LINK = jnp.bfloat16
MESH = pl.DeviceIdType.MESH
F32 = jnp.float32
BF16 = jnp.bfloat16


def dot(left, right, dims):
    return lax.dot_general(left, right, (dims, ((), ())), preferred_element_type=F32)


def split(value):
    high = value.astype(BF16)
    return high, (value - high.astype(F32)).astype(BF16)


def exclusive(left, right, size):
    result, bit = 0, 1
    while bit < size:
        result = result + bit * lax.rem(lax.div(left, bit) + lax.div(right, bit), 2)
        bit *= 2
    return result


def when(condition, body):
    if isinstance(condition, bool):
        if condition:
            body()
    else:
        pl.when(condition)(body)


def pack(moments, half):
    real = moments[:half, :half] + moments[half:, half:]
    imag = moments[:half, half:] - moments[half:, :half]
    row = lax.broadcasted_iota(jnp.int32, (half, half), 0)
    col = lax.broadcasted_iota(jnp.int32, (half, half), 1)
    return jnp.where(row <= col, real, imag)


def unpack(packed, half):
    row = lax.broadcasted_iota(jnp.int32, (half, half), 0)
    col = lax.broadcasted_iota(jnp.int32, (half, half), 1)
    other = packed.T
    real = jnp.where(row <= col, packed, other)
    imag = jnp.where(row > col, packed, jnp.where(row < col, -other, 0.0))
    return real, imag


def orthonormal(real, imag):
    shape = real.shape
    row = lax.broadcasted_iota(jnp.int32, shape, 0)

    def spread(value, k):
        return jnp.broadcast_to(value[k : k + 1, :], shape)

    table = []
    for k in range(KMAX):
        a_re, a_im = spread(real, k), spread(imag, k)
        s_re = jnp.sum(a_re * real + a_im * imag, axis=1, keepdims=True)
        s_im = jnp.sum(a_re * imag - a_im * real, axis=1, keepdims=True)
        table.append((jnp.broadcast_to(s_re, shape), jnp.broadcast_to(s_im, shape)))
    for k in range(KMAX):
        s_re, s_im = table[k]
        inverse = lax.rsqrt(jnp.maximum(spread(s_re, k), 0.0) + EPS)
        square = inverse * inverse
        a_re, a_im = spread(real, k), spread(imag, k)
        c_re, c_im = s_re * square, s_im * square
        later_re = real - c_re * a_re + c_im * a_im
        later_im = imag - c_re * a_im - c_im * a_re
        real = jnp.where(row > k, later_re, jnp.where(row == k, real * inverse, real))
        imag = jnp.where(row > k, later_im, jnp.where(row == k, imag * inverse, imag))
        factor = 1.0 + EPS * square
        d_re, d_im = c_re * factor, c_im * factor
        for m in range(k + 1, KMAX):
            m_re, m_im = spread(d_re, m), spread(d_im, m)
            t_re, t_im = table[m]
            table[m] = (
                t_re - (m_re * s_re + m_im * s_im),
                t_im - (m_re * s_im - m_im * s_re),
            )
    return real, imag


def apply_operator(operator, real, imag, half):
    high, low = split(jnp.concatenate([real, imag], axis=0))
    left = jnp.concatenate([high, high, low], axis=1)
    image = dot(left, operator, ((1,), (0,)))
    new_re = image[:KMAX, :half] + image[KMAX:, half:]
    new_im = image[KMAX:, :half] - image[:KMAX, half:]
    return new_re, new_im


def select(crosses, side, partner, groups):
    per = 128 // ROWS
    lane = lax.broadcasted_iota(jnp.int32, (ROWS, 128), 1)
    place = lax.rem(lax.broadcasted_iota(jnp.int32, (KMAX, 128), 1), ROWS)
    parts = []
    for first in range(0, groups, per):
        kept = jnp.zeros((ROWS, 128), F32)
        for f in range(first, first + per):
            block = crosses[side, partner[side, f]]
            kept = jnp.where(lax.div(lane, ROWS) == f - first, block[:, first * ROWS : first * ROWS + 128], kept)
        top, bottom = kept[:KMAX], kept[KMAX:]
        real = top + pltpu.roll(bottom, 128 - KMAX, 1)
        imag = pltpu.roll(bottom, KMAX, 1) - top
        parts.append(jnp.where(place < KMAX, real, imag))
    return jnp.concatenate(parts, axis=1)


def kernel(
    n_freq, n_space, spectra, weight_in, partner_in, counts_in,
    modes, energy_out, coherence_out,
    ring, held, weight, relay, relayed, kept, send, recv, mine_sum, coefs, energies, mirrored, scaled,
    crosses, partner_there, partials, arrived, partner, counts,
    load_sem, small_sem, relay_send, relay_recv, gram_send, gram_recv, basis_send, basis_recv,
    energy_send, energy_recv, modes_send, modes_recv, partner_send, partner_recv, part_send, part_recv,
):
    groups, width, points = held.shape
    half = width // 2
    part = points // 2
    own = groups // n_space
    chips = n_space // 2
    wide = groups * ROWS
    total = points * n_space
    band = lax.axis_index("freq")
    me = lax.axis_index("space")
    opposite = n_freq - 1 - band
    peers = [exclusive(me, apart, n_space) for apart in range(n_space)]
    beside = peers[1]
    upper = jnp.where(band > opposite, 1, 0)
    mine = pl.multiple_of(upper * part, 128)
    theirs = pl.multiple_of((1 - upper) * part, 128)

    def order(step):
        owner = exclusive(me, n_space - 1 - lax.rem(step, n_space), n_space)
        return lax.div(step, n_space) * n_space + owner

    def load(step):
        place = lax.rem(step, AHEAD)
        return pltpu.make_async_copy(spectra.at[order(step)], ring.at[place], load_sem.at[place])

    weight_copy = pltpu.make_async_copy(weight_in, weight, small_sem.at[0])
    weight_copy.start()
    for step in range(2):
        load(step).start()

    barrier = pltpu.get_barrier_semaphore()
    for apart in range(1, n_space):
        peer = lax.rem(me + apart, n_space)
        pl.semaphore_signal(barrier, inc=1, device_id=(band, peer), device_id_type=MESH)
    for apart in range(n_space):
        peer = lax.rem(me + apart, n_space)
        pl.semaphore_signal(barrier, inc=1, device_id=(opposite, peer), device_id_type=MESH)

    mine_copy = pltpu.make_async_copy(partner_in, partner.at[pl.ds(0, 1)], small_sem.at[1])
    counts_copy = pltpu.make_async_copy(counts_in, counts, small_sem.at[2])
    mine_copy.start()
    counts_copy.start()
    weight_copy.wait()
    for step in range(2, 4):
        load(step).start()

    def gram_pair(pair):
        packed = []
        for step in (2 * pair, 2 * pair + 1):
            load(step).wait()

        def more():
            load(2 * pair + 4).start()
            load(2 * pair + 5).start()

        when(2 * pair + 4 < groups, more)

        for step in (2 * pair, 2 * pair + 1):
            block = ring[lax.rem(step, AHEAD)]
            flipped = block.T
            held[order(step)] = flipped
            weighted = (flipped.astype(F32) * weight[...]).astype(BF16)
            packed.append(pack(dot(weighted, block, ((1,), (0,))), half))
        relay[pair] = packed[0]
        kept[pair] = packed[1]

    def relay_copy(pair):
        return pltpu.make_async_remote_copy(
            src_ref=relay.at[pair], dst_ref=relayed.at[pair], send_sem=relay_send,
            recv_sem=relay_recv.at[pair], device_id=(band, beside), device_id_type=MESH,
        )

    def gram_copy(slot, place):
        peer = exclusive(me, n_space - 2 - 2 * place, n_space)
        return pltpu.make_async_remote_copy(
            src_ref=send.at[slot, place], dst_ref=recv.at[slot, place], send_sem=gram_send,
            recv_sem=gram_recv.at[slot], device_id=(band, peer), device_id_type=MESH,
        )

    def forward(pair):
        if isinstance(pair, int):
            slot, place = pair // chips, pair % chips
        else:
            slot, place = lax.div(pair, chips), lax.rem(pair, chips)
        relay_copy(pair).wait_recv()
        chip = kept[pair] + relayed[pair]

        def away():
            send[slot, place] = chip.astype(LINK)
            gram_copy(slot, place).start()

        def here():
            mine_sum[slot] = chip

        when(place < chips - 1, away)
        when(place == chips - 1, here)

    def gram_step(pair, carry):
        gram_pair(pair)
        relay_copy(pair).start()
        forward(pair - 1)
        return carry

    gram_pair(0)
    pl.semaphore_wait(barrier, 2 * n_space - 1)
    relay_copy(0).start()
    partner_copy = pltpu.make_async_remote_copy(
        src_ref=partner_in, dst_ref=partner_there, send_sem=partner_send,
        recv_sem=partner_recv, device_id=(opposite, me), device_id_type=MESH,
    )
    partner_copy.start()
    mine_copy.wait()
    counts_copy.wait()

    pairs = own * chips
    rest = chips // 2 if own > 1 else 0
    for pair in range(1, pairs - rest):
        gram_step(pair, 0)
    if not rest:
        forward(pairs - 1)

    def basis_copy(f, peer):
        return pltpu.make_async_remote_copy(
            src_ref=coefs.at[f], dst_ref=coefs.at[f], send_sem=basis_send,
            recv_sem=basis_recv.at[f], device_id=(band, peer), device_id_type=MESH,
        )

    def energy_copy(span, peer):
        return pltpu.make_async_remote_copy(
            src_ref=energies.at[span], dst_ref=energies.at[span], send_sem=energy_send,
            recv_sem=energy_recv, device_id=(band, peer), device_id_type=MESH,
        )

    def solve(slot):
        f = slot * n_space + me
        pltpu.make_async_remote_copy(
            src_ref=send.at[slot], dst_ref=recv.at[slot], send_sem=gram_send,
            recv_sem=gram_recv.at[slot], device_id=(band, beside), device_id_type=MESH,
        ).wait_recv()
        packed = mine_sum[slot]
        for place in range(chips - 1):
            packed = packed + recv[slot, place].astype(F32)
        real, imag = unpack(packed / total, half)
        high, low = split(jnp.concatenate([real, imag], axis=1))
        operator = jnp.concatenate([high, low, high], axis=0)
        real, imag = orthonormal(real[:KMAX], -imag[:KMAX])
        for _ in range(ITERS - 1):
            real, imag = orthonormal(*apply_operator(operator, real, imag, half))
        image_re, image_im = apply_operator(operator, real, imag, half)
        energy = jnp.sum(real * image_re + imag * image_im, axis=1, keepdims=True)
        energy = jnp.broadcast_to(energy, (KMAX, half))
        rank = lax.broadcasted_iota(jnp.int32, (KMAX, half), 0)
        scale = jnp.where(rank < counts[0, f], 1.0 / jnp.sqrt(energy + EPS), 0.0)
        coefs[f] = jnp.concatenate([real * scale, imag * scale], axis=0).astype(BF16)
        energies[f] = energy
        for peer in reversed(peers[1:]):
            basis_copy(f, peer).start()

    def modes_copy(f):
        return pltpu.make_async_remote_copy(
            src_ref=modes.at[f, :, pl.ds(theirs, part)], dst_ref=mirrored.at[f],
            send_sem=modes_send, recv_sem=modes_recv.at[lax.div(f, n_space)],
            device_id=(opposite, me), device_id_type=MESH,
        )

    def modes_step(slot, step):
        source = peers[step] if isinstance(step, int) else exclusive(me, step, n_space)
        f = slot * n_space + source

        when(step > 0, lambda: basis_copy(f, source).wait_recv())

        basis = coefs[f].astype(F32)
        real, imag = basis[:KMAX], basis[KMAX:]
        coefficient = jnp.concatenate(
            [jnp.concatenate([real, -imag], axis=1), jnp.concatenate([imag, real], axis=1)], axis=0
        ).astype(BF16)
        modes[f] = dot(coefficient, held[f], ((1,), (0,))).astype(BF16)
        modes_copy(f).start()
        weighted = modes[f, :, pl.ds(mine, part)].astype(F32) * weight[:, pl.ds(mine, part)]
        scaled[f] = weighted.astype(BF16)

    for slot in range(own):
        solve(slot)
        modes_step(slot, 0)
        for peer in reversed(peers[1:]):
            energy_copy(pl.ds(slot * n_space + me, 1), peer).start()

        def alone(step, carry, slot=slot):
            modes_step(slot, step)
            return carry

        if slot == 0 and rest:

            def both(turn, carry):
                lax.fori_loop(jnp.maximum(2 * turn, 1), 2 * turn + 2, alone, 0)
                return gram_step(pairs - rest + turn, carry)

            lax.fori_loop(0, rest, both, 0)
            lax.fori_loop(2 * rest, 2 * rest + 2, alone, 0)
            forward(pairs - 1)
            lax.fori_loop(2 * rest + 2, n_space, alone, 0)
        else:
            lax.fori_loop(1, n_space, alone, 0)

    partner_copy.wait()
    there_copy = pltpu.make_async_copy(partner_there, partner.at[pl.ds(1, 1)], small_sem.at[1])
    there_copy.start()
    sent = pl.ds(0, own * (n_space - 1))
    energy_copy(sent, beside).wait()
    lane = lax.broadcasted_iota(jnp.int32, (KMAX, half), 1)
    gathered = jnp.zeros((KMAX, half), F32)
    for f in range(groups):
        gathered = jnp.where(lane == f, energies[f], gathered)
    energy_out[...] = gathered
    pltpu.make_async_remote_copy(
        src_ref=coefs.at[sent], dst_ref=coefs.at[sent], send_sem=basis_send,
        recv_sem=basis_recv.at[0], device_id=(band, beside), device_id_type=MESH,
    ).wait_send()
    pltpu.make_async_remote_copy(
        src_ref=relay, dst_ref=relayed, send_sem=relay_send,
        recv_sem=relay_recv.at[0], device_id=(band, beside), device_id_type=MESH,
    ).wait_send()
    pltpu.make_async_remote_copy(
        src_ref=send, dst_ref=recv, send_sem=gram_send,
        recv_sem=gram_recv.at[0], device_id=(band, beside), device_id_type=MESH,
    ).wait_send()
    there_copy.wait()

    for slot in range(own):
        span = pl.ds(slot * n_space, n_space)
        pltpu.make_async_remote_copy(
            src_ref=mirrored.at[span], dst_ref=mirrored.at[span], send_sem=modes_send,
            recv_sem=modes_recv.at[slot], device_id=(opposite, me), device_id_type=MESH,
        ).wait_recv()
        rows = n_space * ROWS
        psi = mirrored[span].reshape(rows, part)
        cross = dot(scaled[...].reshape(wide, part), psi, ((1,), (1,))) / total
        crosses[0, span] = cross.T.reshape(n_space, ROWS, wide)
        crosses[1, :, :, slot * rows : (slot + 1) * rows] = cross.reshape(groups, ROWS, rows)
    partials[1] = select(crosses, 1, partner, groups).astype(LINK)
    partial = select(crosses, 0, partner, groups)
    partials[0] = partial.astype(LINK)

    def part_copy(side, peer):
        across = opposite if side else band
        return pltpu.make_async_remote_copy(
            src_ref=partials.at[side], dst_ref=arrived.at[side * n_space + me],
            send_sem=part_send, recv_sem=part_recv, device_id=(across, peer), device_id_type=MESH,
        )

    for apart in range(n_space - 1, -1, -1):
        part_copy(1, peers[apart]).start()
        if apart:
            part_copy(0, peers[apart]).start()

    arrived[me] = jnp.zeros(arrived.shape[1:], LINK)
    pltpu.make_async_remote_copy(
        src_ref=mirrored, dst_ref=mirrored, send_sem=modes_send,
        recv_sem=modes_recv.at[0], device_id=(opposite, me), device_id_type=MESH,
    ).wait_send()
    there = pl.ds(0, 2 * n_space - 1)
    pltpu.make_async_remote_copy(
        src_ref=arrived.at[there], dst_ref=arrived.at[there], send_sem=part_send,
        recv_sem=part_recv, device_id=(band, beside), device_id_type=MESH,
    ).wait()
    result = partial
    for place in range(2 * n_space):
        result = result + arrived[place].astype(F32)
    coherence_out[...] = result


def finish(modes, energy, coherence, modes_out, energy_out, coherence_out, few, blocks, sems):
    groups = energy_out.shape[1]
    wide = groups * ROWS
    modes_copy = pltpu.make_async_copy(modes, modes_out, sems.at[2])
    modes_copy.start()
    few[...] = energy[:, :groups]
    energy_copy = pltpu.make_async_copy(few, energy_out, sems.at[0])
    energy_copy.start()
    value = coherence[...]
    high, low = split(value)
    lowest = (value - high.astype(F32) - low.astype(F32)).astype(BF16)
    row = lax.broadcasted_iota(jnp.int32, (wide, wide), 0)
    col = lax.broadcasted_iota(jnp.int32, (wide, wide), 1)
    source = lax.rem(col, groups) * ROWS + lax.div(col, groups)
    move = jnp.where(row == source, 1.0, 0.0).astype(BF16)
    moved = dot(high, move, ((1,), (0,))) + dot(low, move, ((1,), (0,))) + dot(lowest, move, ((1,), (0,)))
    for place in range(ROWS):
        blocks[place] = moved[:, place * groups : (place + 1) * groups]
    coherence_copy = pltpu.make_async_copy(blocks, coherence_out, sems.at[1])
    coherence_copy.start()
    energy_copy.wait()
    coherence_copy.wait()
    modes_copy.wait()


def on_device(n_freq, n_space, spectra, weight, partner, counts):
    groups, points, width = spectra.shape
    half = width // 2
    own = groups // n_space
    wide = groups * ROWS
    dma = pltpu.SemaphoreType.DMA
    vmem = pl.BlockSpec(memory_space=pltpu.VMEM)
    hbm = pl.BlockSpec(memory_space=pltpu.HBM)
    modes, energy, coherence = pl.pallas_call(
        functools.partial(kernel, n_freq, n_space),
        out_shape=(
            pltpu.VMEM((groups, ROWS, points), BF16),
            pltpu.VMEM((KMAX, half), F32),
            pltpu.VMEM((KMAX, wide), F32),
        ),
        in_specs=[hbm, hbm, hbm, hbm],
        out_specs=(vmem, vmem, vmem),
        scratch_shapes=[
            pltpu.VMEM((AHEAD, points, width), BF16),
            pltpu.VMEM((groups, width, points), BF16),
            pltpu.VMEM((1, points), F32),
            pltpu.VMEM((groups // 2, half, half), F32),
            pltpu.VMEM((groups // 2, half, half), F32),
            pltpu.VMEM((groups // 2, half, half), F32),
            pltpu.VMEM((own, n_space // 2 - 1, half, half), LINK),
            pltpu.VMEM((own, n_space // 2 - 1, half, half), LINK),
            pltpu.VMEM((own, half, half), F32),
            pltpu.VMEM((groups, ROWS, half), BF16),
            pltpu.VMEM((groups, KMAX, half), F32),
            pltpu.VMEM((groups, ROWS, points // 2), BF16),
            pltpu.VMEM((groups, ROWS, points // 2), BF16),
            pltpu.VMEM((2, groups, ROWS, wide), F32),
            pltpu.VMEM((1, groups), jnp.int32),
            pltpu.VMEM((2, KMAX, wide), LINK),
            pltpu.VMEM((2 * n_space, KMAX, wide), LINK),
            pltpu.SMEM((2, groups), jnp.int32),
            pltpu.SMEM((1, groups), jnp.int32),
            dma((AHEAD,)),
            dma((3,)),
            dma(()),
            dma((groups // 2,)),
            dma(()),
            dma((own,)),
            dma(()),
            dma((groups,)),
            dma(()),
            dma(()),
            dma(()),
            dma((own,)),
            dma(()),
            dma(()),
            dma(()),
            dma(()),
        ],
        compiler_params=pltpu.CompilerParams(
            collective_id=0, has_side_effects=True, vmem_limit_bytes=60 * 1024 * 1024
        ),
    )(spectra, weight.reshape(1, points), partner.reshape(1, groups), counts.reshape(1, groups))
    modes = pltpu.with_memory_space_constraint(modes, pltpu.VMEM)
    energy = pltpu.with_memory_space_constraint(energy, pltpu.VMEM)
    coherence = pltpu.with_memory_space_constraint(coherence, pltpu.VMEM)
    modes, energy, coherence = pl.pallas_call(
        finish,
        out_shape=(
            jax.ShapeDtypeStruct((groups, ROWS, points), BF16),
            jax.ShapeDtypeStruct((KMAX, groups), F32),
            jax.ShapeDtypeStruct((ROWS, KMAX, groups), F32),
        ),
        in_specs=[vmem, vmem, vmem],
        out_specs=(hbm, hbm, hbm),
        scratch_shapes=[
            pltpu.VMEM((KMAX, groups), F32),
            pltpu.VMEM((ROWS, KMAX, groups), F32),
            dma((3,)),
        ],
    )(modes, energy, coherence)
    coherence = coherence.reshape(2, KMAX, KMAX, groups).transpose(3, 0, 1, 2)
    return modes, energy.T, coherence


def solution(mesh):
    in_specs = (P("freq", "space", None), P("space"), P("freq"), P("freq"))
    out_specs = (P("freq", None, "space"), P("freq", None), P("freq", None, None, None))
    return jax.shard_map(
        functools.partial(on_device, mesh.shape["freq"], mesh.shape["space"]),
        mesh=mesh,
        in_specs=in_specs,
        out_specs=out_specs,
        check_vma=False,
    )
```

```python
import functools

import jax
import jax.numpy as jnp
from jax import lax
from jax.experimental import pallas as pl
from jax.experimental.pallas import tpu as pltpu
from jax.sharding import PartitionSpec as P

KMAX = 8
ROWS = 2 * KMAX
ITERS = 4
AHEAD = 6
EPS = 1e-06
LINK = jnp.bfloat16
MESH = pl.DeviceIdType.MESH
F32 = jnp.float32
BF16 = jnp.bfloat16


def dot(left, right, dims):
    return lax.dot_general(left, right, (dims, ((), ())), preferred_element_type=F32)


def split(value):
    high = value.astype(BF16)
    return high, (value - high.astype(F32)).astype(BF16)


def exclusive(left, right, size):
    result, bit = 0, 1
    while bit < size:
        result = result + bit * lax.rem(lax.div(left, bit) + lax.div(right, bit), 2)
        bit *= 2
    return result


def when(condition, body):
    if isinstance(condition, bool):
        if condition:
            body()
    else:
        pl.when(condition)(body)


def pack(moments, half):
    real = moments[:half, :half] + moments[half:, half:]
    imag = moments[:half, half:] - moments[half:, :half]
    row = lax.broadcasted_iota(jnp.int32, (half, half), 0)
    col = lax.broadcasted_iota(jnp.int32, (half, half), 1)
    return jnp.where(row <= col, real, imag)


def unpack(packed, half):
    row = lax.broadcasted_iota(jnp.int32, (half, half), 0)
    col = lax.broadcasted_iota(jnp.int32, (half, half), 1)
    other = packed.T
    real = jnp.where(row <= col, packed, other)
    imag = jnp.where(row > col, packed, jnp.where(row < col, -other, 0.0))
    return real, imag


def orthonormal(real, imag):
    shape = real.shape
    row = lax.broadcasted_iota(jnp.int32, shape, 0)

    def spread(value, k):
        return jnp.broadcast_to(value[k : k + 1, :], shape)

    table = []
    for k in range(KMAX):
        a_re, a_im = spread(real, k), spread(imag, k)
        s_re = jnp.sum(a_re * real + a_im * imag, axis=1, keepdims=True)
        s_im = jnp.sum(a_re * imag - a_im * real, axis=1, keepdims=True)
        table.append((jnp.broadcast_to(s_re, shape), jnp.broadcast_to(s_im, shape)))
    for k in range(KMAX):
        s_re, s_im = table[k]
        inverse = lax.rsqrt(jnp.maximum(spread(s_re, k), 0.0) + EPS)
        square = inverse * inverse
        a_re, a_im = spread(real, k), spread(imag, k)
        c_re, c_im = s_re * square, s_im * square
        later_re = real - c_re * a_re + c_im * a_im
        later_im = imag - c_re * a_im - c_im * a_re
        real = jnp.where(row > k, later_re, jnp.where(row == k, real * inverse, real))
        imag = jnp.where(row > k, later_im, jnp.where(row == k, imag * inverse, imag))
        factor = 1.0 + EPS * square
        d_re, d_im = c_re * factor, c_im * factor
        for m in range(k + 1, KMAX):
            m_re, m_im = spread(d_re, m), spread(d_im, m)
            t_re, t_im = table[m]
            table[m] = (
                t_re - (m_re * s_re + m_im * s_im),
                t_im - (m_re * s_im - m_im * s_re),
            )
    return real, imag


def apply_operator(operator, real, imag, half):
    high, low = split(jnp.concatenate([real, imag], axis=0))
    left = jnp.concatenate([high, high, low], axis=1)
    image = dot(left, operator, ((1,), (0,)))
    new_re = image[:KMAX, :half] + image[KMAX:, half:]
    new_im = image[KMAX:, :half] - image[:KMAX, half:]
    return new_re, new_im


def select(crosses, side, partner, groups):
    per = 128 // ROWS
    lane = lax.broadcasted_iota(jnp.int32, (ROWS, 128), 1)
    place = lax.rem(lax.broadcasted_iota(jnp.int32, (KMAX, 128), 1), ROWS)
    parts = []
    for first in range(0, groups, per):
        kept = jnp.zeros((ROWS, 128), F32)
        for f in range(first, first + per):
            block = crosses[side, partner[side, f]]
            kept = jnp.where(lax.div(lane, ROWS) == f - first, block[:, first * ROWS : first * ROWS + 128], kept)
        top, bottom = kept[:KMAX], kept[KMAX:]
        real = top + pltpu.roll(bottom, 128 - KMAX, 1)
        imag = pltpu.roll(bottom, KMAX, 1) - top
        parts.append(jnp.where(place < KMAX, real, imag))
    return jnp.concatenate(parts, axis=1)


def kernel(
    n_freq, n_space, spectra, weight_in, partner_in, counts_in,
    modes, energy_out, coherence_out,
    ring, held, weight, relay, relayed, kept, send, recv, mine_sum, coefs, energies, mirrored, scaled,
    crosses, partner_there, partials, arrived, partner, counts,
    load_sem, small_sem, relay_send, relay_recv, gram_send, gram_recv, basis_send, basis_recv,
    energy_send, energy_recv, modes_send, modes_recv, partner_send, partner_recv, part_send, part_recv,
):
    groups, width, points = held.shape
    half = width // 2
    part = points // 2
    own = groups // n_space
    chips = n_space // 2
    wide = groups * ROWS
    total = points * n_space
    band = lax.axis_index("freq")
    me = lax.axis_index("space")
    opposite = n_freq - 1 - band
    peers = [exclusive(me, apart, n_space) for apart in range(n_space)]
    beside = peers[1]
    upper = jnp.where(band > opposite, 1, 0)
    mine = pl.multiple_of(upper * part, 128)
    theirs = pl.multiple_of((1 - upper) * part, 128)

    def order(step):
        owner = exclusive(me, n_space - 1 - lax.rem(step, n_space), n_space)
        return lax.div(step, n_space) * n_space + owner

    def load(step):
        place = lax.rem(step, AHEAD)
        return pltpu.make_async_copy(spectra.at[order(step)], ring.at[place], load_sem.at[place])

    weight_copy = pltpu.make_async_copy(weight_in, weight, small_sem.at[0])
    weight_copy.start()
    for step in range(2):
        load(step).start()

    barrier = pltpu.get_barrier_semaphore()
    for apart in range(1, n_space):
        peer = lax.rem(me + apart, n_space)
        pl.semaphore_signal(barrier, inc=1, device_id=(band, peer), device_id_type=MESH)
    for apart in range(n_space):
        peer = lax.rem(me + apart, n_space)
        pl.semaphore_signal(barrier, inc=1, device_id=(opposite, peer), device_id_type=MESH)

    mine_copy = pltpu.make_async_copy(partner_in, partner.at[pl.ds(0, 1)], small_sem.at[1])
    counts_copy = pltpu.make_async_copy(counts_in, counts, small_sem.at[2])
    mine_copy.start()
    counts_copy.start()
    weight_copy.wait()
    for step in range(2, 4):
        load(step).start()

    def gram_pair(pair):
        packed = []
        for step in (2 * pair, 2 * pair + 1):
            load(step).wait()

        def more():
            load(2 * pair + 4).start()
            load(2 * pair + 5).start()

        when(2 * pair + 4 < groups, more)

        for step in (2 * pair, 2 * pair + 1):
            block = ring[lax.rem(step, AHEAD)]
            flipped = block.T
            held[order(step)] = flipped
            weighted = (flipped.astype(F32) * weight[...]).astype(BF16)
            packed.append(pack(dot(weighted, block, ((1,), (0,))), half))
        relay[pair] = packed[0]
        kept[pair] = packed[1]

    def relay_copy(pair):
        return pltpu.make_async_remote_copy(
            src_ref=relay.at[pair], dst_ref=relayed.at[pair], send_sem=relay_send,
            recv_sem=relay_recv.at[pair], device_id=(band, beside), device_id_type=MESH,
        )

    def gram_copy(slot, place):
        peer = exclusive(me, n_space - 2 - 2 * place, n_space)
        return pltpu.make_async_remote_copy(
            src_ref=send.at[slot, place], dst_ref=recv.at[slot, place], send_sem=gram_send,
            recv_sem=gram_recv.at[slot], device_id=(band, peer), device_id_type=MESH,
        )

    def forward(pair):
        if isinstance(pair, int):
            slot, place = pair // chips, pair % chips
        else:
            slot, place = lax.div(pair, chips), lax.rem(pair, chips)
        relay_copy(pair).wait_recv()
        chip = kept[pair] + relayed[pair]

        def away():
            send[slot, place] = chip.astype(LINK)
            gram_copy(slot, place).start()

        def here():
            mine_sum[slot] = chip

        when(place < chips - 1, away)
        when(place == chips - 1, here)

    def gram_step(pair, carry):
        gram_pair(pair)
        relay_copy(pair).start()
        forward(pair - 1)
        return carry

    gram_pair(0)
    pl.semaphore_wait(barrier, 2 * n_space - 1)
    relay_copy(0).start()
    partner_copy = pltpu.make_async_remote_copy(
        src_ref=partner_in, dst_ref=partner_there, send_sem=partner_send,
        recv_sem=partner_recv, device_id=(opposite, me), device_id_type=MESH,
    )
    partner_copy.start()
    mine_copy.wait()
    counts_copy.wait()

    pairs = own * chips
    rest = chips // 2 if own > 1 else 0
    for pair in range(1, pairs - rest):
        gram_step(pair, 0)
    if not rest:
        forward(pairs - 1)

    def basis_copy(f, peer):
        return pltpu.make_async_remote_copy(
            src_ref=coefs.at[f], dst_ref=coefs.at[f], send_sem=basis_send,
            recv_sem=basis_recv.at[f], device_id=(band, peer), device_id_type=MESH,
        )

    def energy_copy(span, peer):
        return pltpu.make_async_remote_copy(
            src_ref=energies.at[span], dst_ref=energies.at[span], send_sem=energy_send,
            recv_sem=energy_recv, device_id=(band, peer), device_id_type=MESH,
        )

    def solve(slot):
        f = slot * n_space + me
        pltpu.make_async_remote_copy(
            src_ref=send.at[slot], dst_ref=recv.at[slot], send_sem=gram_send,
            recv_sem=gram_recv.at[slot], device_id=(band, beside), device_id_type=MESH,
        ).wait_recv()
        packed = mine_sum[slot]
        for place in range(chips - 1):
            packed = packed + recv[slot, place].astype(F32)
        real, imag = unpack(packed / total, half)
        high, low = split(jnp.concatenate([real, imag], axis=1))
        operator = jnp.concatenate([high, low, high], axis=0)
        real, imag = orthonormal(real[:KMAX], -imag[:KMAX])
        for _ in range(ITERS - 1):
            real, imag = orthonormal(*apply_operator(operator, real, imag, half))
        image_re, image_im = apply_operator(operator, real, imag, half)
        energy = jnp.sum(real * image_re + imag * image_im, axis=1, keepdims=True)
        energy = jnp.broadcast_to(energy, (KMAX, half))
        rank = lax.broadcasted_iota(jnp.int32, (KMAX, half), 0)
        scale = jnp.where(rank < counts[0, f], 1.0 / jnp.sqrt(energy + EPS), 0.0)
        coefs[f] = jnp.concatenate([real * scale, imag * scale], axis=0).astype(BF16)
        energies[f] = energy
        for peer in reversed(peers[1:]):
            basis_copy(f, peer).start()

    def modes_copy(f):
        return pltpu.make_async_remote_copy(
            src_ref=modes.at[f, :, pl.ds(theirs, part)], dst_ref=mirrored.at[f],
            send_sem=modes_send, recv_sem=modes_recv.at[lax.div(f, n_space)],
            device_id=(opposite, me), device_id_type=MESH,
        )

    def modes_step(slot, step):
        source = peers[step] if isinstance(step, int) else exclusive(me, step, n_space)
        f = slot * n_space + source

        when(step > 0, lambda: basis_copy(f, source).wait_recv())

        basis = coefs[f].astype(F32)
        real, imag = basis[:KMAX], basis[KMAX:]
        coefficient = jnp.concatenate(
            [jnp.concatenate([real, -imag], axis=1), jnp.concatenate([imag, real], axis=1)], axis=0
        ).astype(BF16)
        if isinstance(step, int):
            for first in (theirs, mine):
                span = pl.ds(first, part)
                modes[f, :, span] = dot(coefficient, held[f, :, span], ((1,), (0,))).astype(BF16)
                if first is theirs:
                    modes_copy(f).start()
        else:
            modes[f] = dot(coefficient, held[f], ((1,), (0,))).astype(BF16)
            modes_copy(f).start()
        weighted = modes[f, :, pl.ds(mine, part)].astype(F32) * weight[:, pl.ds(mine, part)]
        scaled[f] = weighted.astype(BF16)

    for slot in range(own):
        solve(slot)
        modes_step(slot, 0)
        for peer in reversed(peers[1:]):
            energy_copy(pl.ds(slot * n_space + me, 1), peer).start()

        def alone(step, carry, slot=slot):
            modes_step(slot, step)
            return carry

        if slot == 0 and rest:

            def both(turn, carry):
                lax.fori_loop(jnp.maximum(2 * turn, 1), 2 * turn + 2, alone, 0)
                return gram_step(pairs - rest + turn, carry)

            lax.fori_loop(0, rest, both, 0)
            lax.fori_loop(2 * rest, 2 * rest + 2, alone, 0)
            forward(pairs - 1)
            lax.fori_loop(2 * rest + 2, n_space, alone, 0)
        else:
            lax.fori_loop(1, n_space, alone, 0)

    partner_copy.wait()
    there_copy = pltpu.make_async_copy(partner_there, partner.at[pl.ds(1, 1)], small_sem.at[1])
    there_copy.start()
    sent = pl.ds(0, own * (n_space - 1))
    energy_copy(sent, beside).wait()
    lane = lax.broadcasted_iota(jnp.int32, (KMAX, half), 1)
    gathered = jnp.zeros((KMAX, half), F32)
    for f in range(groups):
        gathered = jnp.where(lane == f, energies[f], gathered)
    energy_out[...] = gathered
    pltpu.make_async_remote_copy(
        src_ref=coefs.at[sent], dst_ref=coefs.at[sent], send_sem=basis_send,
        recv_sem=basis_recv.at[0], device_id=(band, beside), device_id_type=MESH,
    ).wait_send()
    pltpu.make_async_remote_copy(
        src_ref=relay, dst_ref=relayed, send_sem=relay_send,
        recv_sem=relay_recv.at[0], device_id=(band, beside), device_id_type=MESH,
    ).wait_send()
    pltpu.make_async_remote_copy(
        src_ref=send, dst_ref=recv, send_sem=gram_send,
        recv_sem=gram_recv.at[0], device_id=(band, beside), device_id_type=MESH,
    ).wait_send()
    there_copy.wait()

    for slot in range(own):
        span = pl.ds(slot * n_space, n_space)
        pltpu.make_async_remote_copy(
            src_ref=mirrored.at[span], dst_ref=mirrored.at[span], send_sem=modes_send,
            recv_sem=modes_recv.at[slot], device_id=(opposite, me), device_id_type=MESH,
        ).wait_recv()
        rows = n_space * ROWS
        psi = mirrored[span].reshape(rows, part)
        cross = dot(scaled[...].reshape(wide, part), psi, ((1,), (1,))) / total
        crosses[0, span] = cross.T.reshape(n_space, ROWS, wide)
        crosses[1, :, :, slot * rows : (slot + 1) * rows] = cross.reshape(groups, ROWS, rows)
    partials[1] = select(crosses, 1, partner, groups).astype(LINK)

    def part_copy(side, peer):
        across = opposite if side else band
        return pltpu.make_async_remote_copy(
            src_ref=partials.at[side], dst_ref=arrived.at[side * n_space + me],
            send_sem=part_send, recv_sem=part_recv, device_id=(across, peer), device_id_type=MESH,
        )

    for apart in range(n_space - 1, -1, -1):
        part_copy(1, peers[apart]).start()
    partial = select(crosses, 0, partner, groups)
    partials[0] = partial.astype(LINK)
    for apart in range(n_space - 1, 0, -1):
        part_copy(0, peers[apart]).start()

    arrived[me] = jnp.zeros(arrived.shape[1:], LINK)
    pltpu.make_async_remote_copy(
        src_ref=mirrored, dst_ref=mirrored, send_sem=modes_send,
        recv_sem=modes_recv.at[0], device_id=(opposite, me), device_id_type=MESH,
    ).wait_send()
    there = pl.ds(0, 2 * n_space - 1)
    pltpu.make_async_remote_copy(
        src_ref=arrived.at[there], dst_ref=arrived.at[there], send_sem=part_send,
        recv_sem=part_recv, device_id=(band, beside), device_id_type=MESH,
    ).wait()
    result = partial
    for place in range(2 * n_space):
        result = result + arrived[place].astype(F32)
    coherence_out[...] = result


def finish(modes, energy, coherence, modes_out, energy_out, coherence_out, few, blocks, sems):
    groups = energy_out.shape[1]
    wide = groups * ROWS
    modes_copy = pltpu.make_async_copy(modes, modes_out, sems.at[2])
    modes_copy.start()
    few[...] = energy[:, :groups]
    energy_copy = pltpu.make_async_copy(few, energy_out, sems.at[0])
    energy_copy.start()
    value = coherence[...]
    high, low = split(value)
    lowest = (value - high.astype(F32) - low.astype(F32)).astype(BF16)
    row = lax.broadcasted_iota(jnp.int32, (wide, wide), 0)
    col = lax.broadcasted_iota(jnp.int32, (wide, wide), 1)
    source = lax.rem(col, groups) * ROWS + lax.div(col, groups)
    move = jnp.where(row == source, 1.0, 0.0).astype(BF16)
    moved = dot(high, move, ((1,), (0,))) + dot(low, move, ((1,), (0,))) + dot(lowest, move, ((1,), (0,)))
    for place in range(ROWS):
        blocks[place] = moved[:, place * groups : (place + 1) * groups]
    coherence_copy = pltpu.make_async_copy(blocks, coherence_out, sems.at[1])
    coherence_copy.start()
    energy_copy.wait()
    coherence_copy.wait()
    modes_copy.wait()


def on_device(n_freq, n_space, spectra, weight, partner, counts):
    groups, points, width = spectra.shape
    half = width // 2
    own = groups // n_space
    wide = groups * ROWS
    dma = pltpu.SemaphoreType.DMA
    vmem = pl.BlockSpec(memory_space=pltpu.VMEM)
    hbm = pl.BlockSpec(memory_space=pltpu.HBM)
    modes, energy, coherence = pl.pallas_call(
        functools.partial(kernel, n_freq, n_space),
        out_shape=(
            pltpu.VMEM((groups, ROWS, points), BF16),
            pltpu.VMEM((KMAX, half), F32),
            pltpu.VMEM((KMAX, wide), F32),
        ),
        in_specs=[hbm, hbm, hbm, hbm],
        out_specs=(vmem, vmem, vmem),
        scratch_shapes=[
            pltpu.VMEM((AHEAD, points, width), BF16),
            pltpu.VMEM((groups, width, points), BF16),
            pltpu.VMEM((1, points), F32),
            pltpu.VMEM((groups // 2, half, half), F32),
            pltpu.VMEM((groups // 2, half, half), F32),
            pltpu.VMEM((groups // 2, half, half), F32),
            pltpu.VMEM((own, n_space // 2 - 1, half, half), LINK),
            pltpu.VMEM((own, n_space // 2 - 1, half, half), LINK),
            pltpu.VMEM((own, half, half), F32),
            pltpu.VMEM((groups, ROWS, half), BF16),
            pltpu.VMEM((groups, KMAX, half), F32),
            pltpu.VMEM((groups, ROWS, points // 2), BF16),
            pltpu.VMEM((groups, ROWS, points // 2), BF16),
            pltpu.VMEM((2, groups, ROWS, wide), F32),
            pltpu.VMEM((1, groups), jnp.int32),
            pltpu.VMEM((2, KMAX, wide), LINK),
            pltpu.VMEM((2 * n_space, KMAX, wide), LINK),
            pltpu.SMEM((2, groups), jnp.int32),
            pltpu.SMEM((1, groups), jnp.int32),
            dma((AHEAD,)),
            dma((3,)),
            dma(()),
            dma((groups // 2,)),
            dma(()),
            dma((own,)),
            dma(()),
            dma((groups,)),
            dma(()),
            dma(()),
            dma(()),
            dma((own,)),
            dma(()),
            dma(()),
            dma(()),
            dma(()),
        ],
        compiler_params=pltpu.CompilerParams(
            collective_id=0, has_side_effects=True, vmem_limit_bytes=60 * 1024 * 1024
        ),
    )(spectra, weight.reshape(1, points), partner.reshape(1, groups), counts.reshape(1, groups))
    modes = pltpu.with_memory_space_constraint(modes, pltpu.VMEM)
    energy = pltpu.with_memory_space_constraint(energy, pltpu.VMEM)
    coherence = pltpu.with_memory_space_constraint(coherence, pltpu.VMEM)
    modes, energy, coherence = pl.pallas_call(
        finish,
        out_shape=(
            jax.ShapeDtypeStruct((groups, ROWS, points), BF16),
            jax.ShapeDtypeStruct((KMAX, groups), F32),
            jax.ShapeDtypeStruct((ROWS, KMAX, groups), F32),
        ),
        in_specs=[vmem, vmem, vmem],
        out_specs=(hbm, hbm, hbm),
        scratch_shapes=[
            pltpu.VMEM((KMAX, groups), F32),
            pltpu.VMEM((ROWS, KMAX, groups), F32),
            dma((3,)),
        ],
    )(modes, energy, coherence)
    coherence = coherence.reshape(2, KMAX, KMAX, groups).transpose(3, 0, 1, 2)
    return modes, energy.T, coherence


def solution(mesh):
    in_specs = (P("freq", "space", None), P("space"), P("freq"), P("freq"))
    out_specs = (P("freq", None, "space"), P("freq", None), P("freq", None, None, None))
    return jax.shard_map(
        functools.partial(on_device, mesh.shape["freq"], mesh.shape["space"]),
        mesh=mesh,
        in_specs=in_specs,
        out_specs=out_specs,
        check_vma=False,
    )
```
